256 devices in a mesh: shard: 32 (over y, x, core), dp: 8 (over z).
Axes of the slice: x: 4, y: 4, z: 8, core: 2. Of those that a mesh axis runs over, the one named last changes fastest.
Arguments:
- grad: float32 [288, 128, 4096], P('shard', 'dp'), may hold values from -252 to 252
- param: bfloat16 [288, 128, 4096], P('shard', 'dp'), may hold values from -0.119628906 to 0.119628906
- row_state: float32 [288, 128], P('shard', 'dp'), may hold values from 0.3 to 27
- col_state: float32 [3, 4096], replicated, may hold values from 0.002 to 400
- block_start: int32 [32], replicated, may hold values from 0 to 143, as said below
- block_matrix: int32 [144], replicated, may hold values from 0 to 2, as said below
- step: int32 [1], replicated, may hold values from 2 to 11
Outputs:
- new_params: bfloat16 [18432, 4096], P(None, 'shard')
- new_row_state: float32 [288, 128], P('shard', 'dp')
- new_col_state: float32 [3, 4096], replicated
The draws below stay inside these ranges and needn't reach their ends.
Inputs may be any that keep to these rules, and one draw needn't show every extreme that they name: block_start rises from 0 at index 0; every shard index owns between 1 and 9 consecutive global blocks, held in its first slots, and some index owns exactly 9; slots past a device's owned count hold values that no output reads. `block_matrix`: ids 0 and 1 each label 4096 / 128 blocks and id 2 labels 10240 / 128 blocks, in any order.
All inputs are finite; a program needn't handle non-finite values.
Results may differ from the reference program's by a relative error of at most 0.0004.
Values may be sent and summed in bfloat16 or wider, within the bound.
A program may use at most 64 MiB of HBM per device.

```python
import math
import jax
import jax.numpy as jnp
from jax import lax

D = 4096
FF = 10240
BLOCK = 128
MATS = 3
NB = 144
CAP = 9
N_SHARD = 32


def draw_grad(key, part):
    noise_key, row_key, col_key = jax.random.split(jax.random.fold_in(key, 11), 3)
    slot_total = N_SHARD * CAP
    draw_base = jnp.clip(jax.random.normal(noise_key, (slot_total, BLOCK, D), jnp.float32), -4.0, 4.0)
    row_scale = jnp.exp(jax.random.uniform(row_key, (slot_total, BLOCK), jnp.float32, math.log(0.3), math.log(3.0)))
    col_scale = jnp.exp(jax.random.uniform(col_key, (D,), jnp.float32, math.log(0.3), math.log(3.0)))
    position = jnp.arange(slot_total, dtype=jnp.float32) / max(slot_total - 1, 1)
    ramp_scale = 1.0 + 2.0 * position
    return draw_base * (row_scale * ramp_scale[:, None])[:, :, None] * col_scale[None, None, :]


def draw_row_state(key, part):
    slot_total = N_SHARD * CAP
    state_key = jax.random.fold_in(key, 23)
    position = jnp.arange(slot_total, dtype=jnp.float32) / max(slot_total - 1, 1)
    values = jnp.exp(jax.random.uniform(state_key, (slot_total, BLOCK), jnp.float32, math.log(0.3), math.log(3.0)))
    ramp_scale = 1.0 + 2.0 * position
    return values * ramp_scale[:, None]


def draw_col_state(key, part):
    state_key = jax.random.fold_in(key, 37)
    lowest = jnp.array([0.002, 64.0, 0.002], jnp.float32)
    factor = jnp.exp(jax.random.uniform(state_key, (MATS, D), jnp.float32, 0.0, math.log(4.0)))
    return lowest[:, None] * factor


def draw_block_matrix(key, part):
    order_key = jax.random.fold_in(key, 41)
    block_index = jnp.arange(NB, dtype=jnp.int32)
    first_end = D // BLOCK
    second_end = 2 * (D // BLOCK)
    labels = (block_index >= first_end).astype(jnp.int32) + (block_index >= second_end).astype(jnp.int32)
    return jax.random.permutation(order_key, labels).astype(jnp.int32)


def draw_block_start(key, part):
    busy_key, move_key = jax.random.split(jax.random.fold_in(key, 53))
    busy_device = jax.random.randint(busy_key, (), 0, N_SHARD - 1)
    last_device = N_SHARD - 1
    rest_blocks = NB - CAP - 1
    base_count = rest_blocks // (N_SHARD - 2)
    extra_count = rest_blocks % (N_SHARD - 2)
    device_ids = jnp.arange(N_SHARD, dtype=jnp.int32)
    position_rank = device_ids - (device_ids > busy_device).astype(jnp.int32)
    spread_count = base_count + (position_rank < extra_count).astype(jnp.int32)
    counts = jnp.where(device_ids == busy_device, CAP, jnp.where(device_ids == last_device, 1, spread_count)).astype(jnp.int32)

    def move(turn, counts):
        turn_key = jax.random.fold_in(move_key, turn)
        pair_key, amount_key = jax.random.split(turn_key)
        ends_pair = jax.random.randint(pair_key, (2,), 0, N_SHARD)
        source = ends_pair[0]
        target = ends_pair[1]
        wanted = jax.random.randint(amount_key, (), 0, CAP)
        usable = (source != busy_device) & (target != busy_device) & (source != target) & (source != last_device) & (target != last_device)
        amount = jnp.minimum(jnp.minimum(wanted, counts[source] - 1), CAP - counts[target])
        amount = jnp.where(usable, jnp.maximum(amount, 0), 0).astype(jnp.int32)
        return counts.at[source].add(-amount).at[target].add(amount)
    counts = lax.fori_loop(0, 4 * N_SHARD, move, counts)
    return (jnp.cumsum(counts) - counts).astype(jnp.int32)


def levels(stream_key, dims, pieces, least, largest):
    gain = 1.0
    for axis_at, parts in pieces:
        draws = jax.random.uniform(jax.random.fold_in(jax.random.fold_in(stream_key, 6), axis_at), (parts,), jnp.float32, least / len(pieces), largest / len(pieces))
        gain = gain * jnp.repeat(jnp.exp(draws), dims[axis_at] // parts).reshape((-1,) + (1,) * (len(dims) - 1 - axis_at))
    return gain


def normal_values(stream_key, shape, width, limit, shards=(), kind=jnp.bfloat16):
    values = width * jax.random.normal(stream_key, shape, jnp.float32)
    if shards:
        values = values * levels(stream_key, shape, shards, -0.22, 0.18)
    return jnp.clip(values, -limit, limit).astype(kind)


def setup_inputs(seed: int = 0) -> dict:
    streams_of = jax.random.split(jax.random.key(seed), 8)
    return {
        "grad": draw_grad(jax.random.fold_in(streams_of[7], 71), 0),
        "param": normal_values(streams_of[1], (N_SHARD * CAP, BLOCK, D), 0.02, 0.119628906, ((0, 32), (1, 8))),
        "row_state": draw_row_state(jax.random.fold_in(streams_of[7], 71), 0),
        "col_state": draw_col_state(jax.random.fold_in(streams_of[7], 71), 0),
        "block_start": draw_block_start(jax.random.fold_in(streams_of[7], 71), 0),
        "block_matrix": draw_block_matrix(jax.random.fold_in(streams_of[7], 71), 0),
        "step": jax.random.randint(streams_of[6], (1,), 2, 12).astype(jnp.int32),
    }


def scale_grad(grad, safe_rows, matrix_pick, new_cols, row_avg):
    slot_cols = jnp.dot(matrix_pick, new_cols, precision=lax.Precision.HIGHEST)
    slot_avg = jnp.dot(matrix_pick, row_avg, precision=lax.Precision.HIGHEST)
    return grad / jnp.sqrt(safe_rows[:, :, None] * slot_cols[:, None, :] / slot_avg[:, None, None])

def reference(grad, param, row_state, col_state, block_start, block_matrix, step):
    slot_total = grad.shape[0]
    block_ends = jnp.concatenate([block_start[1:], jnp.full((1,), NB, jnp.int32)])
    slot_ids = jnp.arange(slot_total, dtype=jnp.int32)
    owner_shard = slot_ids // CAP
    within = slot_ids % CAP
    owned_count = (block_ends - block_start)[owner_shard]
    live_slot = within < owned_count
    block_ids = jnp.minimum(block_start[owner_shard] + within, NB - 1).astype(jnp.int32)
    matrix_ids = jnp.where(live_slot, block_matrix[block_ids], 0)
    matrix_pick = (matrix_ids[:, None] == jnp.arange(3, dtype=jnp.int32)[None, :]).astype(jnp.float32)
    member = matrix_pick * live_slot[:, None].astype(jnp.float32)
    row_count = jnp.array([D, D, FF], jnp.float32)
    step_value = step[0].astype(jnp.float32)
    decay_rate = 1.0 - step_value ** (-0.8)
    learn_rate = 1.0 / jnp.sqrt(jnp.maximum(step_value, 10000.0))
    squares = grad * grad
    new_rows = jnp.where(live_slot[:, None], decay_rate * row_state + (1.0 - decay_rate) * lax.optimization_barrier(jnp.sum(squares, axis=2)) / D, 0.0)
    safe_rows = jnp.where(live_slot[:, None], new_rows, 1.0)
    col_total = jnp.einsum('sm,sd->md', member, lax.optimization_barrier(jnp.sum(squares, axis=1)), precision=lax.Precision.HIGHEST)
    new_cols = decay_rate * col_state + (1.0 - decay_rate) * col_total / row_count[:, None]
    row_avg = jnp.dot(lax.optimization_barrier(jnp.sum(new_rows, axis=1)), member, precision=lax.Precision.HIGHEST) / row_count
    scaled = scale_grad(grad, safe_rows, matrix_pick, new_cols, row_avg)
    square_total = jnp.dot(lax.optimization_barrier(jnp.sum(scaled * scaled, axis=(1, 2))), member, precision=lax.Precision.HIGHEST)
    clip_factor = jnp.maximum(1.0, jnp.sqrt(square_total / (row_count * D)))
    slot_clip = jnp.dot(matrix_pick, clip_factor, precision=lax.Precision.HIGHEST)
    updated = jnp.where(live_slot[:, None, None], param.astype(jnp.float32) - learn_rate * scaled / slot_clip[:, None, None], 0.0).astype(jnp.bfloat16)
    block_index = jnp.arange(NB, dtype=jnp.int32)
    block_owner = lax.optimization_barrier(jnp.sum((block_start[None, :] <= block_index[:, None]).astype(jnp.int32), axis=1)) - 1
    slot_of = (block_owner * CAP + block_index - jnp.take(block_start, block_owner)).astype(jnp.int32)
    new_params = jnp.take(updated, slot_of, axis=0).reshape(NB * BLOCK, D)
    return (new_params, new_rows, new_cols)
```

```python
import functools

import jax
import jax.numpy as jnp
from jax import lax
from jax.experimental import pallas as pl
from jax.experimental.pallas import tpu as pltpu
from jax.sharding import PartitionSpec as P

MESH = pl.DeviceIdType.MESH
LANES = 128
ROWS = 16
MATS = 3
CHUNKS = 2
PART = ROWS // CHUNKS


def whole_wait(ref, sem):
    pltpu.make_async_copy(ref, ref, sem).wait()


def kernel(
    ns,
    nz,
    cap,
    nb,
    starts,
    mats,
    step,
    grad_hbm,
    param_hbm,
    row_state,
    col_state,
    out_hbm,
    out_rows,
    out_cols,
    g,
    p,
    stat,
    from_plane,
    mine,
    from_line,
    totals,
    row_inv,
    row_fac,
    col_fac,
    updated,
    arrived_0,
    arrived_1,
    pieces,
    slot_of,
    weight,
    matrix_of,
    load_sem,
    small_send,
    small_recv,
    swap_send,
    swap_recv,
    ring_send,
    ring_recv,
    store_sem,
):
    me = lax.axis_index("shard")
    z = lax.axis_index("dp")
    cols = ns * LANES
    f32 = jnp.float32
    half = nb // 2
    last = nz // 2 - 1
    arrived = (arrived_0, arrived_1)

    loads = [pltpu.make_async_copy(grad_hbm, g, load_sem.at[0]), pltpu.make_async_copy(param_hbm, p, load_sem.at[1])]
    for load in loads:
        load.start()
    barrier = pltpu.get_barrier_semaphore()

    @pl.loop(1, ns)
    def _(k):
        pl.semaphore_signal(barrier, inc=1, device_id={"shard": lax.rem(me + k, ns)}, device_id_type=MESH)

    @pl.loop(1, nz)
    def _(k):
        pl.semaphore_signal(barrier, inc=1, device_id={"dp": lax.rem(z + k, nz)}, device_id_type=MESH)

    first = starts[me]
    owned = jnp.where(me == ns - 1, nb, starts[jnp.minimum(me + 1, ns - 1)]) - first
    for j in range(cap):
        m_of = jnp.clip(mats[jnp.minimum(first + j, nb - 1)], 0, MATS - 1)
        matrix_of[j] = m_of
        for m in range(MATS):
            weight[j * MATS + m] = jnp.where((j < owned) & (m_of == m), 1.0, 0.0).astype(f32)

    def place(b, owner):
        following = starts[jnp.minimum(owner + 1, ns - 1)]
        owner = jnp.where((owner < ns - 1) & (following <= b), owner + 1, owner)
        slot_of[b] = owner * cap + jnp.clip(b - starts[owner], 0, cap - 1)
        return owner

    lax.fori_loop(0, nb, place, jnp.int32(0))

    t = jnp.full((ROWS, LANES), step[0].astype(f32), f32)
    beta = 1.0 - jnp.exp(-0.8 * jnp.log(t))
    rest = 1.0 - beta
    lr = 1.0 / jnp.sqrt(jnp.maximum(t, 10000.0))
    sub = lax.broadcasted_iota(jnp.int32, (ROWS, ROWS), 0)
    lane = lax.broadcasted_iota(jnp.int32, (ROWS, ROWS), 1)
    eye = sub == lane

    loads[0].wait()
    row_sums = [jnp.zeros((ROWS, 1), f32) for _ in range(MATS)]
    for j in range(cap):
        gj = g[j]
        total = jnp.sum(gj * gj, axis=1, keepdims=True)
        live = jnp.full((ROWS, 1), owned, jnp.int32) > j
        old = jnp.sum(jnp.where(eye, jnp.broadcast_to(row_state[j : j + 1, :], (ROWS, ROWS)), 0.0), axis=1, keepdims=True)
        new = jnp.where(live, beta[:, :1] * old + rest[:, :1] * total / cols, 0.0)
        safe = jnp.where(live, new, 1.0)
        row_inv[j] = jnp.broadcast_to(1.0 / safe, (ROWS, LANES))
        row_fac[j] = jnp.broadcast_to(1.0 / jnp.sqrt(safe), (ROWS, LANES))
        out_rows[j : j + 1, :] = jnp.sum(jnp.where(eye, jnp.broadcast_to(new, (ROWS, ROWS)), 0.0), axis=0, keepdims=True)
        for m in range(MATS):
            row_sums[m] = row_sums[m] + weight[j * MATS + m] * new
    at_lane = lax.broadcasted_iota(jnp.int32, (1, LANES), 1)
    row_line = jnp.zeros((1, LANES), f32)
    for m in range(MATS):
        row_line = jnp.where(at_lane == m, jnp.sum(row_sums[m], axis=0, keepdims=True), row_line)

    @pl.loop(0, ns)
    def _(q):
        at = pl.ds(pl.multiple_of(q * LANES, LANES), LANES)
        acc = [jnp.zeros((8, LANES), f32) for _ in range(2 * MATS)]
        for j in range(cap):
            upper = g[j, 0:8, at]
            lower = g[j, 8:16, at]
            upper, lower = upper * upper, lower * lower
            plain = upper + lower
            quot = upper * row_inv[j, 0:8] + lower * row_inv[j, 8:16]
            for m in range(MATS):
                w = weight[j * MATS + m]
                acc[m] = acc[m] + w * plain
                acc[MATS + m] = acc[MATS + m] + w * quot
        for i in range(2 * MATS):
            stat[q, i : i + 1, :] = jnp.sum(acc[i], axis=0, keepdims=True)
        stat[q, 6:7, :] = row_line
        stat[q, 7:8, :] = jnp.zeros((1, LANES), f32)

    pl.semaphore_wait(barrier, ns - 1 + nz - 1)

    from_plane[me] = stat[me]

    @pl.loop(1, ns)
    def _(k):
        q = lax.rem(me + k, ns)
        pltpu.make_async_remote_copy(
            stat.at[q], from_plane.at[me], small_send.at[0], small_recv.at[0], device_id={"shard": q}, device_id_type=MESH
        ).start()

    whole_wait(from_plane.at[pl.ds(0, ns - 1)], small_recv.at[0])
    parts = [from_plane[s] for s in range(4)]
    for s in range(4, ns):
        parts[s % 4] = parts[s % 4] + from_plane[s]
    mine[0] = (parts[0] + parts[1]) + (parts[2] + parts[3])
    from_line[z] = mine[0]

    @pl.loop(1, nz)
    def _(k):
        other = lax.rem(z + k, nz)
        pltpu.make_async_remote_copy(
            mine.at[0], from_line.at[z], small_send.at[1], small_recv.at[1], device_id={"dp": other}, device_id_type=MESH
        ).start()

    whole_wait(from_line.at[pl.ds(0, nz - 1)], small_recv.at[1])
    both = from_line[0]
    for s in range(1, nz):
        both = both + from_line[s]
    mine[1] = both
    totals[me] = both

    @pl.loop(1, ns)
    def _(k):
        q = lax.rem(me + k, ns)
        pltpu.make_async_remote_copy(
            mine.at[1], totals.at[me], small_send.at[2], small_recv.at[2], device_id={"shard": q}, device_id_type=MESH
        ).start()

    loads[1].wait()
    whole_wait(totals.at[pl.ds(0, ns - 1)], small_recv.at[2])

    row_count = jnp.where(lax.broadcasted_iota(jnp.int32, (MATS, LANES), 0) < 2, f32(cols), f32(nb * ROWS * nz - 2 * cols))
    ratio = jnp.zeros((MATS, LANES), f32)
    for q in range(ns):
        at = pl.ds(q * LANES, LANES)
        new = beta[:MATS] * col_state[:, at] + rest[:MATS] * totals[q, 0:MATS, :] / row_count
        out_cols[:, at] = new
        ratio = ratio + totals[q, MATS : 2 * MATS, :] / new
    ratio = jnp.sum(ratio, axis=1, keepdims=True)
    spread = jnp.broadcast_to(totals[0, 6:7, :], (8, LANES))
    on = lax.broadcasted_iota(jnp.int32, (8, LANES), 0) == lax.broadcasted_iota(jnp.int32, (8, LANES), 1)
    row_total = jnp.sum(jnp.where(on, spread, 0.0), axis=1, keepdims=True)[:MATS]
    average = row_total / row_count[:, :1]
    clip = jnp.maximum(1.0, jnp.sqrt(average * ratio / (row_count[:, :1] * cols)))
    scale = lr[:MATS, :1] * jnp.sqrt(average) / clip
    for q in range(ns):
        col_fac[q, 0:MATS, :] = scale / jnp.sqrt(out_cols[:, pl.ds(q * LANES, LANES)])

    @pl.loop(0, ns)
    def _(q):
        at = pl.ds(pl.multiple_of(q * LANES, LANES), LANES)
        for j in range(cap):
            factor = col_fac[q, pl.ds(matrix_of[j], 1), :]
            value = p[j, :, at].astype(f32) - g[j, :, at] * row_fac[j] * factor
            for c in range(CHUNKS):
                updated[c, q, j] = value[c * PART : (c + 1) * PART].astype(jnp.bfloat16)

    for c in range(CHUNKS):

        @pl.loop(1, ns)
        def _(k):
            q = lax.rem(me + k, ns)
            pltpu.make_async_remote_copy(
                updated.at[c, q],
                arrived[c].at[pl.ds(me * cap, cap)],
                swap_send.at[c],
                swap_recv.at[c],
                device_id={"shard": q},
                device_id_type=MESH,
            ).start()

        for j in range(cap):
            arrived[c][me * cap + j] = updated[c, me, j]

    def unit(c, origin, h):
        return pieces.at[c * nz + origin, pl.ds(h * half, half)]

    def ring_copy(way, c, s, h):
        origin = lax.rem(z + (nz - s if way == 0 else s), nz)
        to = lax.rem(z + (1 if way == 0 else nz - 1), nz)
        return pltpu.make_async_remote_copy(
            unit(c, origin, h),
            unit(c, origin, h),
            ring_send.at[way],
            ring_recv.at[way, c, s, h],
            device_id={"dp": to},
            device_id_type=MESH,
        )

    def keep(c, origin, h):
        pltpu.make_async_copy(unit(c, origin, h), out_hbm.at[pl.ds(h * half, half), origin, c], store_sem.at[0]).start()

    def compact(c):
        whole_wait(arrived[c].at[pl.ds(0, (ns - 1) * cap)], swap_recv.at[c])
        for h in range(2):

            @pl.loop(h * half, (h + 1) * half, unroll=8)
            def _(b):
                pieces[c * nz + z, b] = arrived[c][slot_of[b]]

            ring_copy(0, c, 0, h).start()
            ring_copy(1, c, 0, h).start()
            keep(c, z, h)

    def take(c, s):
        for h in range(2):
            for way in range(2):
                if s == last and h != way:
                    continue
                origin = lax.rem(z + (nz - 1 - s if way == 0 else 1 + s), nz)
                whole_wait(unit(c, origin, h), ring_recv.at[way, c, s, h])
                if s + 1 < last or (s + 1 == last and h == way):
                    ring_copy(way, c, s + 1, h).start()
                keep(c, origin, h)

    compact(0)
    take(0, 0)
    for c in range(1, CHUNKS):
        compact(c)
        for s in range(1, last + 1):
            take(c - 1, s)
        take(c, 0)
    for s in range(1, last + 1):
        take(CHUNKS - 1, s)

    whole_wait(from_plane.at[pl.ds(0, ns - 1)], small_send.at[0])
    whole_wait(from_line.at[pl.ds(0, nz - 1)], small_send.at[1])
    whole_wait(from_plane.at[pl.ds(0, ns - 1)], small_send.at[2])
    for c in range(CHUNKS):
        whole_wait(arrived[c].at[pl.ds(0, (ns - 1) * cap)], swap_send.at[c])
    for way in range(2):
        whole_wait(pieces.at[pl.ds(0, CHUNKS * last + CHUNKS // 2)], ring_send.at[way])
    whole_wait(out_hbm, store_sem.at[0])


def body(ns, nz, grad, param, row_state, col_state, block_start, block_matrix, step):
    cap = grad.shape[0]
    nb = block_matrix.shape[0]
    f32, bf16 = jnp.float32, jnp.bfloat16
    dma = pltpu.SemaphoreType.DMA
    smem = pl.BlockSpec(memory_space=pltpu.SMEM)
    vmem = pl.BlockSpec(memory_space=pltpu.VMEM)
    anywhere = pl.BlockSpec(memory_space=pl.ANY)
    new_params, new_rows, new_cols = pl.pallas_call(
        functools.partial(kernel, ns, nz, cap, nb),
        out_shape=(
            jax.ShapeDtypeStruct((nb, nz, CHUNKS, PART, LANES), bf16),
            jax.ShapeDtypeStruct(row_state.shape, f32),
            jax.ShapeDtypeStruct(col_state.shape, f32),
        ),
        in_specs=[smem, smem, smem, anywhere, anywhere, vmem, vmem],
        out_specs=(anywhere, vmem, vmem),
        scratch_shapes=[
            pltpu.VMEM(grad.shape, f32),
            pltpu.VMEM(param.shape, bf16),
            pltpu.VMEM((ns, 8, LANES), f32),
            pltpu.VMEM((ns, 8, LANES), f32),
            pltpu.VMEM((2, 8, LANES), f32),
            pltpu.VMEM((nz, 8, LANES), f32),
            pltpu.VMEM((ns, 8, LANES), f32),
            pltpu.VMEM((cap, ROWS, LANES), f32),
            pltpu.VMEM((cap, ROWS, LANES), f32),
            pltpu.VMEM((ns, 8, LANES), f32),
            pltpu.VMEM((CHUNKS, ns, cap, PART, LANES), bf16),
            pltpu.VMEM((ns * cap, PART, LANES), bf16),
            pltpu.VMEM((ns * cap, PART, LANES), bf16),
            pltpu.VMEM((CHUNKS * nz, nb, PART, LANES), bf16),
            pltpu.SMEM((nb,), jnp.int32),
            pltpu.SMEM((cap * MATS,), f32),
            pltpu.SMEM((cap,), jnp.int32),
            dma((2,)),
            dma((3,)),
            dma((3,)),
            dma((CHUNKS,)),
            dma((CHUNKS,)),
            dma((2,)),
            dma((2, CHUNKS, nz // 2, 2)),
            dma((1,)),
        ],
        compiler_params=pltpu.CompilerParams(collective_id=0, has_side_effects=True),
        name="step",
    )(block_start, block_matrix, step, grad, param, row_state, col_state)
    return new_params.reshape(nb * nz * ROWS, LANES), new_rows, new_cols


def solution(mesh):
    return jax.shard_map(
        functools.partial(body, mesh.shape["shard"], mesh.shape["dp"]),
        mesh=mesh,
        in_specs=(P("shard", "dp", None), P("shard", "dp", None), P("shard", "dp"), P(), P(), P(), P()),
        out_specs=(P(None, "shard"), P("shard", "dp"), P()),
        check_vma=False,
    )
```

```python
import functools

import jax
import jax.numpy as jnp
from jax import lax
from jax.experimental import pallas as pl
from jax.experimental.pallas import tpu as pltpu
from jax.sharding import PartitionSpec as P

MESH = pl.DeviceIdType.MESH
LANES = 128
ROWS = 16
MATS = 3
CHUNKS = 4
PART = ROWS // CHUNKS


def whole_wait(ref, sem):
    pltpu.make_async_copy(ref, ref, sem).wait()


def sends(last):
    order = [(c, s) for c in range(CHUNKS) for s in range(last + 1)]
    return sorted(order, key=lambda at: (at[0] * (last + 1) + at[1] - (1.5 if at[1] == 0 else 0), at))


def kernel(
    ns,
    nz,
    cap,
    nb,
    step,
    starts_hbm,
    mats_hbm,
    grad_hbm,
    param_hbm,
    row_state_hbm,
    col_state_hbm,
    pieces,
    out_rows,
    out_cols,
    starts,
    mats,
    row_state,
    col_state,
    g,
    p,
    stat,
    from_plane,
    mine,
    from_line,
    totals,
    row_inv,
    row_fac,
    col_fac,
    updated,
    arrived_0,
    arrived_1,
    arrived_2,
    arrived_3,
    slot_of,
    weight,
    matrix_of,
    load_sem,
    small_send,
    small_recv,
    swap_send,
    swap_recv,
    ring_send,
    ring_recv,
):
    me = lax.axis_index("shard")
    z = lax.axis_index("dp")
    cols = ns * LANES
    f32 = jnp.float32
    half = nb // 2
    last = nz // 2 - 1
    arrived = (arrived_0, arrived_1, arrived_2, arrived_3)

    loads = [
        pltpu.make_async_copy(source, target, load_sem.at[i])
        for i, (source, target) in enumerate(
            (
                (starts_hbm, starts),
                (mats_hbm, mats),
                (row_state_hbm, row_state),
                (grad_hbm, g),
                (col_state_hbm, col_state),
                (param_hbm, p),
            )
        )
    ]
    for load in loads:
        load.start()
    barrier = pltpu.get_barrier_semaphore()

    @pl.loop(1, ns)
    def _(k):
        pl.semaphore_signal(barrier, inc=1, device_id={"shard": lax.rem(me + k, ns)}, device_id_type=MESH)

    @pl.loop(1, nz)
    def _(k):
        pl.semaphore_signal(barrier, inc=1, device_id={"dp": lax.rem(z + k, nz)}, device_id_type=MESH)

    for load in loads[:3]:
        load.wait()
    first = starts[me]
    owned = jnp.where(me == ns - 1, nb, starts[jnp.minimum(me + 1, ns - 1)]) - first
    for j in range(cap):
        m_of = jnp.clip(mats[jnp.minimum(first + j, nb - 1)], 0, MATS - 1)
        matrix_of[j] = m_of
        for m in range(MATS):
            weight[j * MATS + m] = jnp.where((j < owned) & (m_of == m), 1.0, 0.0).astype(f32)

    t = jnp.full((ROWS, LANES), step[0].astype(f32), f32)
    beta = 1.0 - jnp.exp(-0.8 * jnp.log(t))
    rest = 1.0 - beta
    lr = 1.0 / jnp.sqrt(jnp.maximum(t, 10000.0))
    sub = lax.broadcasted_iota(jnp.int32, (ROWS, ROWS), 0)
    lane = lax.broadcasted_iota(jnp.int32, (ROWS, ROWS), 1)
    eye = sub == lane

    loads[3].wait()
    row_sums = [jnp.zeros((ROWS, 1), f32) for _ in range(MATS)]
    for j in range(cap):
        gj = g[j]
        total = jnp.sum(gj * gj, axis=1, keepdims=True)
        live = jnp.full((ROWS, 1), owned, jnp.int32) > j
        old = jnp.sum(jnp.where(eye, jnp.broadcast_to(row_state[j : j + 1, :], (ROWS, ROWS)), 0.0), axis=1, keepdims=True)
        new = jnp.where(live, beta[:, :1] * old + rest[:, :1] * total / cols, 0.0)
        safe = jnp.where(live, new, 1.0)
        row_inv[j] = jnp.broadcast_to(1.0 / safe, (ROWS, LANES))
        row_fac[j] = jnp.broadcast_to(1.0 / jnp.sqrt(safe), (ROWS, LANES))
        out_rows[j : j + 1, :] = jnp.sum(jnp.where(eye, jnp.broadcast_to(new, (ROWS, ROWS)), 0.0), axis=0, keepdims=True)
        for m in range(MATS):
            row_sums[m] = row_sums[m] + weight[j * MATS + m] * new
    at_lane = lax.broadcasted_iota(jnp.int32, (1, LANES), 1)
    row_line = jnp.zeros((1, LANES), f32)
    for m in range(MATS):
        row_line = jnp.where(at_lane == m, jnp.sum(row_sums[m], axis=0, keepdims=True), row_line)

    @pl.loop(0, ns)
    def _(q):
        at = pl.ds(pl.multiple_of(q * LANES, LANES), LANES)
        acc = [jnp.zeros((8, LANES), f32) for _ in range(2 * MATS)]
        for j in range(cap):
            upper = g[j, 0:8, at]
            lower = g[j, 8:16, at]
            upper, lower = upper * upper, lower * lower
            plain = upper + lower
            quot = upper * row_inv[j, 0:8] + lower * row_inv[j, 8:16]
            for m in range(MATS):
                w = weight[j * MATS + m]
                acc[m] = acc[m] + w * plain
                acc[MATS + m] = acc[MATS + m] + w * quot
        for i in range(2 * MATS):
            stat[q, i : i + 1, :] = jnp.sum(acc[i], axis=0, keepdims=True)
        stat[q, 6:7, :] = row_line
        stat[q, 7:8, :] = jnp.zeros((1, LANES), f32)

    pl.semaphore_wait(barrier, ns - 1 + nz - 1)

    from_plane[me] = stat[me]

    @pl.loop(1, ns)
    def _(k):
        q = lax.rem(me + k, ns)
        pltpu.make_async_remote_copy(
            stat.at[q], from_plane.at[me], small_send.at[0], small_recv.at[0], device_id={"shard": q}, device_id_type=MESH
        ).start()

    def place(b, owner):
        following = starts[jnp.minimum(owner + 1, ns - 1)]
        owner = jnp.where((owner < ns - 1) & (following <= b), owner + 1, owner)
        slot_of[b] = owner * cap + jnp.clip(b - starts[owner], 0, cap - 1)
        return owner

    lax.fori_loop(0, nb, place, jnp.int32(0))

    whole_wait(from_plane.at[pl.ds(0, ns - 1)], small_recv.at[0])
    parts = [from_plane[s] for s in range(4)]
    for s in range(4, ns):
        parts[s % 4] = parts[s % 4] + from_plane[s]
    mine[0] = (parts[0] + parts[1]) + (parts[2] + parts[3])
    from_line[z] = mine[0]

    @pl.loop(1, nz)
    def _(k):
        other = lax.rem(z + k, nz)
        pltpu.make_async_remote_copy(
            mine.at[0], from_line.at[z], small_send.at[1], small_recv.at[1], device_id={"dp": other}, device_id_type=MESH
        ).start()

    whole_wait(from_line.at[pl.ds(0, nz - 1)], small_recv.at[1])
    both = from_line[0]
    for s in range(1, nz):
        both = both + from_line[s]
    mine[1] = both
    totals[me] = both

    @pl.loop(1, ns)
    def _(k):
        q = lax.rem(me + k, ns)
        pltpu.make_async_remote_copy(
            mine.at[1], totals.at[me], small_send.at[2], small_recv.at[2], device_id={"shard": q}, device_id_type=MESH
        ).start()

    loads[4].wait()
    loads[5].wait()
    whole_wait(totals.at[pl.ds(0, ns - 1)], small_recv.at[2])

    row_count = jnp.where(lax.broadcasted_iota(jnp.int32, (MATS, LANES), 0) < 2, f32(cols), f32(nb * ROWS * nz - 2 * cols))
    ratio = jnp.zeros((MATS, LANES), f32)
    for q in range(ns):
        at = pl.ds(q * LANES, LANES)
        new = beta[:MATS] * col_state[:, at] + rest[:MATS] * totals[q, 0:MATS, :] / row_count
        out_cols[:, at] = new
        ratio = ratio + totals[q, MATS : 2 * MATS, :] / new
    ratio = jnp.sum(ratio, axis=1, keepdims=True)
    spread = jnp.broadcast_to(totals[0, 6:7, :], (8, LANES))
    on = lax.broadcasted_iota(jnp.int32, (8, LANES), 0) == lax.broadcasted_iota(jnp.int32, (8, LANES), 1)
    row_total = jnp.sum(jnp.where(on, spread, 0.0), axis=1, keepdims=True)[:MATS]
    average = row_total / row_count[:, :1]
    clip = jnp.maximum(1.0, jnp.sqrt(average * ratio / (row_count[:, :1] * cols)))
    scale = lr[:MATS, :1] * jnp.sqrt(average) / clip
    for q in range(ns):
        col_fac[q, 0:MATS, :] = scale / jnp.sqrt(out_cols[:, pl.ds(q * LANES, LANES)])

    @pl.loop(0, ns)
    def _(q):
        at = pl.ds(pl.multiple_of(q * LANES, LANES), LANES)
        for j in range(cap):
            factor = col_fac[q, pl.ds(matrix_of[j], 1), :]
            value = p[j, :, at].astype(f32) - g[j, :, at] * row_fac[j] * factor
            for c in range(CHUNKS):
                updated[c, q, j] = value[c * PART : (c + 1) * PART].astype(jnp.bfloat16)

    for c in range(CHUNKS):

        @pl.loop(1, ns)
        def _(k):
            q = lax.rem(me + k, ns)
            pltpu.make_async_remote_copy(
                updated.at[c, q],
                arrived[c].at[pl.ds(me * cap, cap)],
                swap_send.at[c],
                swap_recv.at[c],
                device_id={"shard": q},
                device_id_type=MESH,
            ).start()

        for j in range(cap):
            arrived[c][me * cap + j] = updated[c, me, j]

    def unit(c, origin, h):
        return pieces.at[c * nz + origin, pl.ds(h * half, half)]

    def ring_copy(way, c, s, h):
        origin = lax.rem(z + (nz - s if way == 0 else s), nz)
        to = lax.rem(z + (1 if way == 0 else nz - 1), nz)
        return pltpu.make_async_remote_copy(
            unit(c, origin, h),
            unit(c, origin, h),
            ring_send.at[way],
            ring_recv.at[way, c, s, h],
            device_id={"dp": to},
            device_id_type=MESH,
        )

    def compact(c):
        whole_wait(arrived[c].at[pl.ds(0, (ns - 1) * cap)], swap_recv.at[c])
        for h in range(2):

            @pl.loop(h * half, (h + 1) * half, unroll=8)
            def _(b):
                pieces[c * nz + z, b] = arrived[c][slot_of[b]]

            ring_copy(0, c, 0, h).start()
            ring_copy(1, c, 0, h).start()

    def take(c, s):
        for h in range(2):
            for way in range(2):
                if s == last and h != way:
                    continue
                origin = lax.rem(z + (nz - 1 - s if way == 0 else 1 + s), nz)
                whole_wait(unit(c, origin, h), ring_recv.at[way, c, s, h])
                if s + 1 < last or (s + 1 == last and h == way):
                    ring_copy(way, c, s + 1, h).start()

    for c, s in sends(last):
        if s == 0:
            compact(c)
        else:
            take(c, s - 1)
    for c in range(CHUNKS):
        take(c, last)

    whole_wait(from_plane.at[pl.ds(0, ns - 1)], small_send.at[0])
    whole_wait(from_line.at[pl.ds(0, nz - 1)], small_send.at[1])
    whole_wait(from_plane.at[pl.ds(0, ns - 1)], small_send.at[2])
    for c in range(CHUNKS):
        whole_wait(arrived[c].at[pl.ds(0, (ns - 1) * cap)], swap_send.at[c])
    for way in range(2):
        whole_wait(pieces.at[pl.ds(0, CHUNKS * last + CHUNKS // 2)], ring_send.at[way])


def finish(nz, pieces, rows, cols, out_params, out_rows, out_cols, sem):
    copies = [
        pltpu.make_async_copy(pieces.at[c * nz + s], out_params.at[:, s, c], sem.at[c * nz + s]) for c in range(CHUNKS) for s in range(nz)
    ]
    copies.append(pltpu.make_async_copy(rows, out_rows, sem.at[CHUNKS * nz]))
    copies.append(pltpu.make_async_copy(cols, out_cols, sem.at[CHUNKS * nz + 1]))
    for copy in copies:
        copy.start()
    for copy in copies:
        copy.wait()


def body(ns, nz, grad, param, row_state, col_state, block_start, block_matrix, step):
    cap = grad.shape[0]
    nb = block_matrix.shape[0]
    f32, bf16 = jnp.float32, jnp.bfloat16
    dma = pltpu.SemaphoreType.DMA
    vmem = pl.BlockSpec(memory_space=pltpu.VMEM)
    hbm = pl.BlockSpec(memory_space=pltpu.HBM)
    landed = pl.pallas_call(
        functools.partial(kernel, ns, nz, cap, nb),
        out_shape=(
            pltpu.VMEM((CHUNKS * nz, nb, PART, LANES), bf16),
            pltpu.VMEM(row_state.shape, f32),
            pltpu.VMEM(col_state.shape, f32),
        ),
        in_specs=[pl.BlockSpec(memory_space=pltpu.SMEM)] + [hbm] * 6,
        out_specs=(vmem, vmem, vmem),
        scratch_shapes=[
            pltpu.SMEM(block_start.shape, jnp.int32),
            pltpu.SMEM(block_matrix.shape, jnp.int32),
            pltpu.VMEM(row_state.shape, f32),
            pltpu.VMEM(col_state.shape, f32),
            pltpu.VMEM(grad.shape, f32),
            pltpu.VMEM(param.shape, bf16),
            pltpu.VMEM((ns, 8, LANES), f32),
            pltpu.VMEM((ns, 8, LANES), f32),
            pltpu.VMEM((2, 8, LANES), f32),
            pltpu.VMEM((nz, 8, LANES), f32),
            pltpu.VMEM((ns, 8, LANES), f32),
            pltpu.VMEM((cap, ROWS, LANES), f32),
            pltpu.VMEM((cap, ROWS, LANES), f32),
            pltpu.VMEM((ns, 8, LANES), f32),
            pltpu.VMEM((CHUNKS, ns, cap, PART, LANES), bf16),
            *[pltpu.VMEM((ns * cap, PART, LANES), bf16) for _ in range(CHUNKS)],
            pltpu.SMEM((nb,), jnp.int32),
            pltpu.SMEM((cap * MATS,), f32),
            pltpu.SMEM((cap,), jnp.int32),
            dma((6,)),
            dma((3,)),
            dma((3,)),
            dma((CHUNKS,)),
            dma((CHUNKS,)),
            dma((2,)),
            dma((2, CHUNKS, nz // 2, 2)),
        ],
        compiler_params=pltpu.CompilerParams(collective_id=0, has_side_effects=True, vmem_limit_bytes=24 << 20),
        name="step",
    )(step, *(pltpu.with_memory_space_constraint(a, pltpu.HBM) for a in (block_start, block_matrix, grad, param, row_state, col_state)))
    new_params, new_rows, new_cols = pl.pallas_call(
        functools.partial(finish, nz),
        out_shape=(
            jax.ShapeDtypeStruct((nb, nz, CHUNKS, PART, LANES), bf16),
            jax.ShapeDtypeStruct(row_state.shape, f32),
            jax.ShapeDtypeStruct(col_state.shape, f32),
        ),
        in_specs=[vmem] * 3,
        out_specs=(hbm,) * 3,
        scratch_shapes=[dma((CHUNKS * nz + 2,))],
        compiler_params=pltpu.CompilerParams(vmem_limit_bytes=8 << 20),
        name="finish",
    )(*landed)
    return new_params.reshape(nb * nz * ROWS, LANES), new_rows, new_cols


def solution(mesh):
    return jax.shard_map(
        functools.partial(body, mesh.shape["shard"], mesh.shape["dp"]),
        mesh=mesh,
        in_specs=(P("shard", "dp", None), P("shard", "dp", None), P("shard", "dp"), P(), P(), P(), P()),
        out_specs=(P(None, "shard"), P("shard", "dp"), P()),
        check_vma=False,
    )
```

```python
import functools

import jax
import jax.numpy as jnp
from jax import lax
from jax.experimental import pallas as pl
from jax.experimental.pallas import tpu as pltpu
from jax.sharding import PartitionSpec as P

MESH = pl.DeviceIdType.MESH
LANES = 128
ROWS = 16
MATS = 3
CHUNKS = 4
UNITS = 4
UNROLL = 6
LATE = 6
PART = ROWS // CHUNKS


def whole_wait(ref, sem):
    pltpu.make_async_copy(ref, ref, sem).wait()


def sends(last):
    order = [(c, s) for c in range(CHUNKS) for s in range(last + 1)]
    return sorted(order, key=lambda at: (3.5 * at[0] + 2 * at[1] - 0.5 if at[0] else at[1] + max(0, at[1] - 2), at))


def kernel(
    ns,
    nz,
    cap,
    nb,
    step,
    starts_hbm,
    mats_hbm,
    grad_hbm,
    param_hbm,
    row_state_hbm,
    col_state_hbm,
    pieces,
    out_rows,
    out_cols,
    starts,
    mats,
    row_state,
    col_state,
    g,
    p,
    stat,
    from_plane,
    mine,
    from_line,
    totals,
    row_inv,
    row_fac,
    col_fac,
    updated,
    early_g,
    early_p,
    came_g,
    came_p,
    arrived_1,
    arrived_2,
    arrived_3,
    slot_of,
    weight,
    matrix_of,
    load_sem,
    small_send,
    small_recv,
    swap_send,
    swap_recv,
    ring_send,
    ring_recv,
):
    me = lax.axis_index("shard")
    z = lax.axis_index("dp")
    cols = ns * LANES
    f32 = jnp.float32
    span = nb // UNITS
    last = nz // 2 - 1
    arrived = (None, arrived_1, arrived_2, arrived_3)

    loads = [
        pltpu.make_async_copy(source, target, load_sem.at[i])
        for i, (source, target) in enumerate(
            (
                (starts_hbm, starts),
                (mats_hbm, mats),
                (row_state_hbm, row_state),
                (grad_hbm, g),
                (col_state_hbm, col_state),
                (param_hbm, p),
            )
        )
    ]
    for load in loads:
        load.start()
    barrier = pltpu.get_barrier_semaphore()

    @pl.loop(1, ns)
    def _(k):
        pl.semaphore_signal(barrier, inc=1, device_id={"shard": lax.rem(me + k, ns)}, device_id_type=MESH)

    @pl.loop(1, nz)
    def _(k):
        pl.semaphore_signal(barrier, inc=1, device_id={"dp": lax.rem(z + k, nz)}, device_id_type=MESH)

    for load in loads[:3]:
        load.wait()
    first = starts[me]
    owned = jnp.where(me == ns - 1, nb, starts[jnp.minimum(me + 1, ns - 1)]) - first
    for j in range(cap):
        m_of = jnp.clip(mats[jnp.minimum(first + j, nb - 1)], 0, MATS - 1)
        matrix_of[j] = m_of
        for m in range(MATS):
            weight[j * MATS + m] = jnp.where((j < owned) & (m_of == m), 1.0, 0.0).astype(f32)

    t = jnp.full((ROWS, LANES), step[0].astype(f32), f32)
    beta = 1.0 - jnp.exp(-0.8 * jnp.log(t))
    rest = 1.0 - beta
    lr = 1.0 / jnp.sqrt(jnp.maximum(t, 10000.0))
    sub = lax.broadcasted_iota(jnp.int32, (ROWS, ROWS), 0)
    lane = lax.broadcasted_iota(jnp.int32, (ROWS, ROWS), 1)
    eye = sub == lane

    loads[3].wait()
    row_sums = [jnp.zeros((ROWS, 1), f32) for _ in range(MATS)]
    for j in range(cap):
        gj = g[j]
        total = jnp.sum(gj * gj, axis=1, keepdims=True)
        live = jnp.full((ROWS, 1), owned, jnp.int32) > j
        old = jnp.sum(jnp.where(eye, jnp.broadcast_to(row_state[j : j + 1, :], (ROWS, ROWS)), 0.0), axis=1, keepdims=True)
        new = jnp.where(live, beta[:, :1] * old + rest[:, :1] * total / cols, 0.0)
        safe = jnp.where(live, new, 1.0)
        row_inv[j] = jnp.broadcast_to(1.0 / safe, (ROWS, LANES))
        row_fac[j] = jnp.broadcast_to(1.0 / jnp.sqrt(safe), (ROWS, LANES))
        out_rows[j : j + 1, :] = jnp.sum(jnp.where(eye, jnp.broadcast_to(new, (ROWS, ROWS)), 0.0), axis=0, keepdims=True)
        for m in range(MATS):
            row_sums[m] = row_sums[m] + weight[j * MATS + m] * new
    at_lane = lax.broadcasted_iota(jnp.int32, (1, LANES), 1)
    row_line = jnp.zeros((1, LANES), f32)
    for m in range(MATS):
        row_line = jnp.where(at_lane == m, jnp.sum(row_sums[m], axis=0, keepdims=True), row_line)

    @pl.loop(0, ns)
    def _(q):
        at = pl.ds(pl.multiple_of(q * LANES, LANES), LANES)
        acc = [jnp.zeros((8, LANES), f32) for _ in range(2 * MATS)]
        for j in range(cap):
            upper = g[j, 0:8, at]
            lower = g[j, 8:16, at]
            upper, lower = upper * upper, lower * lower
            plain = upper + lower
            quot = upper * row_inv[j, 0:8] + lower * row_inv[j, 8:16]
            for m in range(MATS):
                w = weight[j * MATS + m]
                acc[m] = acc[m] + w * plain
                acc[MATS + m] = acc[MATS + m] + w * quot
        for i in range(2 * MATS):
            stat[q, i : i + 1, :] = jnp.sum(acc[i], axis=0, keepdims=True)
        stat[q, 6:7, :] = row_line
        stat[q, 7:8, :] = jnp.zeros((1, LANES), f32)

    pl.semaphore_wait(barrier, ns - 1 + nz - 1)

    from_plane[me] = stat[me]

    @pl.loop(1, ns)
    def _(k):
        q = lax.rem(me + k, ns)
        pltpu.make_async_remote_copy(
            stat.at[q], from_plane.at[me], small_send.at[0], small_recv.at[0], device_id={"shard": q}, device_id_type=MESH
        ).start()

    loads[5].wait()

    def early(q):
        now = cap - LATE
        parts = ((early_g.at[q], me * cap, cap, came_g), (early_p.at[q, pl.ds(0, now)], me * cap, now, came_p))
        parts += ((early_p.at[q, pl.ds(now, LATE)], me * cap + now, LATE, came_p),)
        return [
            pltpu.make_async_remote_copy(
                source, target.at[pl.ds(at, size)], swap_send.at[i], swap_recv.at[i], device_id={"shard": q}, device_id_type=MESH
            )
            for i, (source, at, size, target) in enumerate(parts)
        ]

    def prepare(q, to_g, to_p, first_row):
        at = pl.ds(pl.multiple_of(q * LANES, LANES), LANES)
        for j in range(cap):
            to_g[first_row + j] = (g[j, 0:8, at] * row_fac[j, 0:8])[:PART]
            to_p[first_row + j] = p[j, :, at][:PART]

    prepare(me, came_g, came_p, me * cap)

    @pl.loop(1, ns)
    def _(k):
        q = lax.rem(me + k, ns)
        prepare(q, early_g.at[q], early_p.at[q], 0)
        for copy in early(q)[:2]:
            copy.start()

    def place(b, owner):
        following = starts[jnp.minimum(owner + 1, ns - 1)]
        owner = jnp.where((owner < ns - 1) & (following <= b), owner + 1, owner)
        slot_of[b] = owner * cap + jnp.clip(b - starts[owner], 0, cap - 1)
        return owner

    lax.fori_loop(0, nb, place, jnp.int32(0))

    whole_wait(from_plane.at[pl.ds(0, ns - 1)], small_recv.at[0])
    parts = [from_plane[s] for s in range(4)]
    for s in range(4, ns):
        parts[s % 4] = parts[s % 4] + from_plane[s]
    mine[0] = (parts[0] + parts[1]) + (parts[2] + parts[3])
    from_line[z] = mine[0]

    @pl.loop(1, nz)
    def _(k):
        other = lax.rem(z + k, nz)
        pltpu.make_async_remote_copy(
            mine.at[0], from_line.at[z], small_send.at[1], small_recv.at[1], device_id={"dp": other}, device_id_type=MESH
        ).start()

    whole_wait(from_line.at[pl.ds(0, nz - 1)], small_recv.at[1])
    both = from_line[0]
    for s in range(1, nz):
        both = both + from_line[s]
    mine[1] = both
    totals[me] = both

    @pl.loop(1, ns)
    def _(k):
        q = lax.rem(me + k, ns)
        pltpu.make_async_remote_copy(
            mine.at[1], totals.at[me], small_send.at[2], small_recv.at[2], device_id={"shard": q}, device_id_type=MESH
        ).start()

    @pl.loop(1, ns)
    def _(k):
        early(lax.rem(me + k, ns))[2].start()

    loads[4].wait()
    whole_wait(totals.at[pl.ds(0, ns - 1)], small_recv.at[2])

    row_count = jnp.where(lax.broadcasted_iota(jnp.int32, (MATS, LANES), 0) < 2, f32(cols), f32(nb * ROWS * nz - 2 * cols))
    ratio = jnp.zeros((MATS, LANES), f32)
    for q in range(ns):
        at = pl.ds(q * LANES, LANES)
        new = beta[:MATS] * col_state[:, at] + rest[:MATS] * totals[q, 0:MATS, :] / row_count
        out_cols[:, at] = new
        ratio = ratio + totals[q, MATS : 2 * MATS, :] / new
    ratio = jnp.sum(ratio, axis=1, keepdims=True)
    spread = jnp.broadcast_to(totals[0, 6:7, :], (8, LANES))
    on = lax.broadcasted_iota(jnp.int32, (8, LANES), 0) == lax.broadcasted_iota(jnp.int32, (8, LANES), 1)
    row_total = jnp.sum(jnp.where(on, spread, 0.0), axis=1, keepdims=True)[:MATS]
    average = row_total / row_count[:, :1]
    clip = jnp.maximum(1.0, jnp.sqrt(average * ratio / (row_count[:, :1] * cols)))
    scale = lr[:MATS, :1] * jnp.sqrt(average) / clip
    for q in range(ns):
        col_fac[q, 0:MATS, :] = scale / jnp.sqrt(out_cols[:, pl.ds(q * LANES, LANES)])

    def unit(c, origin, h):
        return pieces.at[c * nz + origin, pl.ds(h * span, span)]

    def ring_copy(way, c, s, h):
        origin = lax.rem(z + (nz - s if way == 0 else s), nz)
        to = lax.rem(z + (1 if way == 0 else nz - 1), nz)
        return pltpu.make_async_remote_copy(
            unit(c, origin, h),
            unit(c, origin, h),
            ring_send.at[way],
            ring_recv.at[way, c, s, h],
            device_id={"dp": to},
            device_id_type=MESH,
        )

    def send_own(c, h):
        ring_copy(0, c, 0, h).start()
        ring_copy(1, c, 0, h).start()

    def goes(way, s, h):
        return s < last or (s == last and h * 2 // UNITS == way)

    whole_wait(came_g.at[pl.ds(0, (ns - 1) * cap)], swap_recv.at[0])
    whole_wait(came_p.at[pl.ds(0, (ns - 1) * (cap - LATE))], swap_recv.at[1])
    whole_wait(came_p.at[pl.ds(0, (ns - 1) * LATE)], swap_recv.at[2])
    for h in range(UNITS):

        @pl.loop(h * span, (h + 1) * span, unroll=UNROLL)
        def _(b):
            slot = slot_of[b]
            factor = col_fac[me, pl.ds(jnp.clip(mats[b], 0, MATS - 1), 1), :]
            pieces[z, b] = (came_p[slot].astype(f32) - came_g[slot] * factor).astype(jnp.bfloat16)

        send_own(0, h)

    @pl.loop(0, ns)
    def _(q):
        at = pl.ds(pl.multiple_of(q * LANES, LANES), LANES)
        for j in range(cap):
            factor = col_fac[q, pl.ds(matrix_of[j], 1), :]
            value = p[j, :, at].astype(f32) - g[j, :, at] * row_fac[j] * factor
            for c in range(1, CHUNKS):
                updated[c - 1, q, j] = value[c * PART : (c + 1) * PART].astype(jnp.bfloat16)

    for c in range(1, CHUNKS):

        @pl.loop(1, ns)
        def _(k):
            q = lax.rem(me + k, ns)
            pltpu.make_async_remote_copy(
                updated.at[c - 1, q],
                arrived[c].at[pl.ds(me * cap, cap)],
                swap_send.at[c + 2],
                swap_recv.at[c + 2],
                device_id={"shard": q},
                device_id_type=MESH,
            ).start()

        for j in range(cap):
            arrived[c][me * cap + j] = updated[c - 1, me, j]

    def compact(c):
        whole_wait(arrived[c].at[pl.ds(0, (ns - 1) * cap)], swap_recv.at[c + 2])
        for h in range(UNITS):

            @pl.loop(h * span, (h + 1) * span, unroll=UNROLL)
            def _(b):
                pieces[c * nz + z, b] = arrived[c][slot_of[b]]

            send_own(c, h)

    def take(c, s):
        for h in range(UNITS):
            for way in range(2):
                if not goes(way, s, h):
                    continue
                origin = lax.rem(z + (nz - 1 - s if way == 0 else 1 + s), nz)
                whole_wait(unit(c, origin, h), ring_recv.at[way, c, s, h])
                if s < last and goes(way, s + 1, h):
                    ring_copy(way, c, s + 1, h).start()

    for c, s in sends(last)[1:]:
        if s == 0:
            compact(c)
        else:
            take(c, s - 1)
    for c in range(CHUNKS):
        take(c, last)

    whole_wait(from_plane.at[pl.ds(0, ns - 1)], small_send.at[0])
    whole_wait(from_line.at[pl.ds(0, nz - 1)], small_send.at[1])
    whole_wait(from_plane.at[pl.ds(0, ns - 1)], small_send.at[2])
    whole_wait(came_g.at[pl.ds(0, (ns - 1) * cap)], swap_send.at[0])
    whole_wait(came_p.at[pl.ds(0, (ns - 1) * (cap - LATE))], swap_send.at[1])
    whole_wait(came_p.at[pl.ds(0, (ns - 1) * LATE)], swap_send.at[2])
    for c in range(1, CHUNKS):
        whole_wait(arrived[c].at[pl.ds(0, (ns - 1) * cap)], swap_send.at[c + 2])
    for way in range(2):
        whole_wait(pieces.at[pl.ds(0, CHUNKS * last + CHUNKS // 2)], ring_send.at[way])


def finish(nz, pieces, rows, cols, out_params, out_rows, out_cols, sem):
    copies = [
        pltpu.make_async_copy(pieces.at[c * nz + s], out_params.at[:, s, c], sem.at[c * nz + s]) for c in range(CHUNKS) for s in range(nz)
    ]
    copies.append(pltpu.make_async_copy(rows, out_rows, sem.at[CHUNKS * nz]))
    copies.append(pltpu.make_async_copy(cols, out_cols, sem.at[CHUNKS * nz + 1]))
    for copy in copies:
        copy.start()
    for copy in copies:
        copy.wait()


def body(ns, nz, grad, param, row_state, col_state, block_start, block_matrix, step):
    cap = grad.shape[0]
    nb = block_matrix.shape[0]
    f32, bf16 = jnp.float32, jnp.bfloat16
    dma = pltpu.SemaphoreType.DMA
    vmem = pl.BlockSpec(memory_space=pltpu.VMEM)
    hbm = pl.BlockSpec(memory_space=pltpu.HBM)
    landed = pl.pallas_call(
        functools.partial(kernel, ns, nz, cap, nb),
        out_shape=(
            pltpu.VMEM((CHUNKS * nz, nb, PART, LANES), bf16),
            pltpu.VMEM(row_state.shape, f32),
            pltpu.VMEM(col_state.shape, f32),
        ),
        in_specs=[pl.BlockSpec(memory_space=pltpu.SMEM)] + [hbm] * 6,
        out_specs=(vmem, vmem, vmem),
        scratch_shapes=[
            pltpu.SMEM(block_start.shape, jnp.int32),
            pltpu.SMEM(block_matrix.shape, jnp.int32),
            pltpu.VMEM(row_state.shape, f32),
            pltpu.VMEM(col_state.shape, f32),
            pltpu.VMEM(grad.shape, f32),
            pltpu.VMEM(param.shape, bf16),
            pltpu.VMEM((ns, 8, LANES), f32),
            pltpu.VMEM((ns, 8, LANES), f32),
            pltpu.VMEM((2, 8, LANES), f32),
            pltpu.VMEM((nz, 8, LANES), f32),
            pltpu.VMEM((ns, 8, LANES), f32),
            pltpu.VMEM((cap, ROWS, LANES), f32),
            pltpu.VMEM((cap, ROWS, LANES), f32),
            pltpu.VMEM((ns, 8, LANES), f32),
            pltpu.VMEM((CHUNKS - 1, ns, cap, PART, LANES), bf16),
            pltpu.VMEM((ns, cap, PART, LANES), f32),
            pltpu.VMEM((ns, cap, PART, LANES), bf16),
            pltpu.VMEM((ns * cap, PART, LANES), f32),
            pltpu.VMEM((ns * cap, PART, LANES), bf16),
            *[pltpu.VMEM((ns * cap, PART, LANES), bf16) for _ in range(CHUNKS - 1)],
            pltpu.SMEM((nb,), jnp.int32),
            pltpu.SMEM((cap * MATS,), f32),
            pltpu.SMEM((cap,), jnp.int32),
            dma((6,)),
            dma((3,)),
            dma((3,)),
            dma((CHUNKS + 2,)),
            dma((CHUNKS + 2,)),
            dma((2,)),
            dma((2, CHUNKS, nz // 2, UNITS)),
        ],
        compiler_params=pltpu.CompilerParams(collective_id=0, has_side_effects=True, vmem_limit_bytes=24 << 20),
        name="step",
    )(step, *(pltpu.with_memory_space_constraint(a, pltpu.HBM) for a in (block_start, block_matrix, grad, param, row_state, col_state)))
    new_params, new_rows, new_cols = pl.pallas_call(
        functools.partial(finish, nz),
        out_shape=(
            jax.ShapeDtypeStruct((nb, nz, CHUNKS, PART, LANES), bf16),
            jax.ShapeDtypeStruct(row_state.shape, f32),
            jax.ShapeDtypeStruct(col_state.shape, f32),
        ),
        in_specs=[vmem] * 3,
        out_specs=(hbm,) * 3,
        scratch_shapes=[dma((CHUNKS * nz + 2,))],
        compiler_params=pltpu.CompilerParams(vmem_limit_bytes=8 << 20),
        name="finish",
    )(*landed)
    return new_params.reshape(nb * nz * ROWS, LANES), new_rows, new_cols


def solution(mesh):
    return jax.shard_map(
        functools.partial(body, mesh.shape["shard"], mesh.shape["dp"]),
        mesh=mesh,
        in_specs=(P("shard", "dp", None), P("shard", "dp", None), P("shard", "dp"), P(), P(), P(), P()),
        out_specs=(P(None, "shard"), P("shard", "dp"), P()),
        check_vma=False,
    )
```

```python
import functools

import jax
import jax.numpy as jnp
from jax import lax
from jax.experimental import pallas as pl
from jax.experimental.pallas import tpu as pltpu
from jax.sharding import PartitionSpec as P

MESH = pl.DeviceIdType.MESH
LANES = 128
ROWS = 16
MATS = 3
PART = 2
SIZES = (1, 1, 2, 4)
FIRST = (0, 1, 2, 4)
CHUNKS = len(SIZES)
UNITS = 4
UNROLL = 6
UPDATE = -1
ORDER = (
    (1, UPDATE),
    (0, 1),
    (2, UPDATE),
    (0, 2),
    (1, 0),
    (3, UPDATE),
    (0, 3),
    (1, 1),
    (2, 0),
    (1, 2),
    (2, 1),
    (1, 3),
    (2, 2),
    (3, 0),
    (2, 3),
    (3, 1),
    (3, 2),
    (3, 3),
)


def whole_wait(ref, sem):
    pltpu.make_async_copy(ref, ref, sem).wait()


def kernel(
    ns,
    nz,
    cap,
    nb,
    step,
    starts_hbm,
    mats_hbm,
    grad_hbm,
    param_hbm,
    row_state_hbm,
    col_state_hbm,
    pieces_0,
    pieces_1,
    pieces_2,
    pieces_3,
    out_rows,
    out_cols,
    starts,
    mats,
    row_state,
    col_state,
    g,
    p,
    stat,
    from_plane,
    mine,
    from_line,
    totals,
    row_inv,
    row_fac,
    col_fac,
    updated_1,
    updated_2,
    updated_3,
    early_g,
    early_p,
    came_g,
    came_p,
    arrived_1,
    arrived_2,
    arrived_3,
    slot_of,
    weight,
    matrix_of,
    load_sem,
    small_send,
    small_recv,
    swap_send,
    swap_recv,
    ring_send,
    ring_recv,
):
    me = lax.axis_index("shard")
    z = lax.axis_index("dp")
    cols = ns * LANES
    f32 = jnp.float32

    def peer(k):
        return lax.rem(me + k, ns)

    span = nb // UNITS
    last = nz // 2 - 1
    pieces = (pieces_0, pieces_1, pieces_2, pieces_3)
    updated = (None, updated_1, updated_2, updated_3)
    arrived = (None, arrived_1, arrived_2, arrived_3)

    loads = [
        pltpu.make_async_copy(source, target, load_sem.at[i])
        for i, (source, target) in enumerate(
            (
                (starts_hbm, starts),
                (mats_hbm, mats),
                (row_state_hbm, row_state),
                (grad_hbm, g),
                (col_state_hbm, col_state),
                (param_hbm, p),
            )
        )
    ]
    for load in loads[:5]:
        load.start()
    barrier = pltpu.get_barrier_semaphore()

    @pl.loop(1, ns)
    def _(k):
        pl.semaphore_signal(barrier, inc=1, device_id={"shard": peer(k)}, device_id_type=MESH)

    @pl.loop(1, nz)
    def _(k):
        pl.semaphore_signal(barrier, inc=1, device_id={"dp": lax.rem(z + k, nz)}, device_id_type=MESH)

    for load in loads[:3]:
        load.wait()
    first = starts[me]
    owned = jnp.where(me == ns - 1, nb, starts[jnp.minimum(me + 1, ns - 1)]) - first
    for j in range(cap):
        m_of = jnp.clip(mats[jnp.minimum(first + j, nb - 1)], 0, MATS - 1)
        matrix_of[j] = m_of
        for m in range(MATS):
            weight[j * MATS + m] = jnp.where((j < owned) & (m_of == m), 1.0, 0.0).astype(f32)

    t = jnp.full((ROWS, LANES), step[0].astype(f32), f32)
    beta = 1.0 - jnp.exp(-0.8 * jnp.log(t))
    rest = 1.0 - beta
    lr = 1.0 / jnp.sqrt(jnp.maximum(t, 10000.0))
    sub = lax.broadcasted_iota(jnp.int32, (ROWS, ROWS), 0)
    lane = lax.broadcasted_iota(jnp.int32, (ROWS, ROWS), 1)
    eye = sub == lane

    loads[3].wait()
    loads[5].start()
    row_sums = [jnp.zeros((ROWS, 1), f32) for _ in range(MATS)]
    for j in range(cap):
        gj = g[j]
        total = jnp.sum(gj * gj, axis=1, keepdims=True)
        live = jnp.full((ROWS, 1), owned, jnp.int32) > j
        old = jnp.sum(jnp.where(eye, jnp.broadcast_to(row_state[j : j + 1, :], (ROWS, ROWS)), 0.0), axis=1, keepdims=True)
        new = jnp.where(live, beta[:, :1] * old + rest[:, :1] * total / cols, 0.0)
        safe = jnp.where(live, new, 1.0)
        row_inv[j] = jnp.broadcast_to(1.0 / safe, (ROWS, LANES))
        row_fac[j] = jnp.broadcast_to(1.0 / jnp.sqrt(safe), (ROWS, LANES))
        out_rows[j : j + 1, :] = jnp.sum(jnp.where(eye, jnp.broadcast_to(new, (ROWS, ROWS)), 0.0), axis=0, keepdims=True)
        for m in range(MATS):
            row_sums[m] = row_sums[m] + weight[j * MATS + m] * new
    at_lane = lax.broadcasted_iota(jnp.int32, (1, LANES), 1)
    row_line = jnp.zeros((1, LANES), f32)
    for m in range(MATS):
        row_line = jnp.where(at_lane == m, jnp.sum(row_sums[m], axis=0, keepdims=True), row_line)

    @pl.loop(0, ns, unroll=4)
    def _(q):
        at = pl.ds(pl.multiple_of(q * LANES, LANES), LANES)
        acc = [jnp.zeros((8, LANES), f32) for _ in range(2 * MATS)]
        for j in range(cap):
            upper = g[j, 0:8, at]
            lower = g[j, 8:16, at]
            upper, lower = upper * upper, lower * lower
            plain = upper + lower
            quot = upper * row_inv[j, 0:8] + lower * row_inv[j, 8:16]
            for m in range(MATS):
                w = weight[j * MATS + m]
                acc[m] = acc[m] + w * plain
                acc[MATS + m] = acc[MATS + m] + w * quot
        for i in range(2 * MATS):
            stat[q, i : i + 1, :] = jnp.sum(acc[i], axis=0, keepdims=True)
        stat[q, 6:7, :] = row_line
        stat[q, 7:8, :] = jnp.zeros((1, LANES), f32)

    pl.semaphore_wait(barrier, ns - 1 + nz - 1)

    from_plane[me] = stat[me]

    @pl.loop(1, ns)
    def _(k):
        q = peer(k)
        pltpu.make_async_remote_copy(
            stat.at[q], from_plane.at[me], small_send.at[0], small_recv.at[0], device_id={"shard": q}, device_id_type=MESH
        ).start()

    loads[5].wait()

    def early(q):
        return [
            pltpu.make_async_remote_copy(
                source.at[q], target.at[pl.ds(me * cap, cap)], swap_send.at[i], swap_recv.at[i], device_id={"shard": q}, device_id_type=MESH
            )
            for i, (source, target) in enumerate(((early_g, came_g), (early_p, came_p)))
        ]

    def prepare(q, to_g, to_p, first_row):
        at = pl.ds(pl.multiple_of(q * LANES, LANES), LANES)
        for j in range(cap):
            to_g[first_row + j] = (g[j, 0:8, at] * row_fac[j, 0:8])[:PART]
            to_p[first_row + j] = p[j, :, at][:PART]

    prepare(me, came_g, came_p, me * cap)

    @pl.loop(1, ns)
    def _(k):
        q = lax.rem(me + k, ns)
        prepare(q, early_g.at[q], early_p.at[q], 0)

    def place(b, owner):
        following = starts[jnp.minimum(owner + 1, ns - 1)]
        owner = jnp.where((owner < ns - 1) & (following <= b), owner + 1, owner)
        slot_of[b] = owner * cap + jnp.clip(b - starts[owner], 0, cap - 1)
        return owner

    lax.fori_loop(0, nb, place, jnp.int32(0))

    whole_wait(from_plane.at[pl.ds(0, ns - 1)], small_recv.at[0])
    parts = [from_plane[s] for s in range(4)]
    for s in range(4, ns):
        parts[s % 4] = parts[s % 4] + from_plane[s]
    mine[0] = (parts[0] + parts[1]) + (parts[2] + parts[3])
    from_line[z] = mine[0]

    @pl.loop(1, nz)
    def _(k):
        other = lax.rem(z + k, nz)
        pltpu.make_async_remote_copy(
            mine.at[0], from_line.at[z], small_send.at[1], small_recv.at[1], device_id={"dp": other}, device_id_type=MESH
        ).start()

    @pl.loop(1, ns)
    def _(k):
        for copy in early(peer(k)):
            copy.start()

    whole_wait(from_line.at[pl.ds(0, nz - 1)], small_recv.at[1])
    both = from_line[0]
    for s in range(1, nz):
        both = both + from_line[s]
    mine[1] = both
    totals[me] = both

    @pl.loop(1, ns)
    def _(k):
        q = peer(k)
        pltpu.make_async_remote_copy(
            mine.at[1], totals.at[me], small_send.at[2], small_recv.at[2], device_id={"shard": q}, device_id_type=MESH
        ).start()

    loads[4].wait()
    whole_wait(totals.at[pl.ds(0, ns - 1)], small_recv.at[2])

    row_count = jnp.where(lax.broadcasted_iota(jnp.int32, (MATS, LANES), 0) < 2, f32(cols), f32(nb * ROWS * nz - 2 * cols))
    ratio = jnp.zeros((MATS, LANES), f32)
    for q in range(ns):
        at = pl.ds(q * LANES, LANES)
        new = beta[:MATS] * col_state[:, at] + rest[:MATS] * totals[q, 0:MATS, :] / row_count
        out_cols[:, at] = new
        ratio = ratio + totals[q, MATS : 2 * MATS, :] / new
    ratio = jnp.sum(ratio, axis=1, keepdims=True)
    spread = jnp.broadcast_to(totals[0, 6:7, :], (8, LANES))
    on = lax.broadcasted_iota(jnp.int32, (8, LANES), 0) == lax.broadcasted_iota(jnp.int32, (8, LANES), 1)
    row_total = jnp.sum(jnp.where(on, spread, 0.0), axis=1, keepdims=True)[:MATS]
    average = row_total / row_count[:, :1]
    clip = jnp.maximum(1.0, jnp.sqrt(average * ratio / (row_count[:, :1] * cols)))
    scale = lr[:MATS, :1] * jnp.sqrt(average) / clip
    for q in range(ns):
        col_fac[q, 0:MATS, :] = scale / jnp.sqrt(out_cols[:, pl.ds(q * LANES, LANES)])

    def unit(c, origin, h):
        return pieces[c].at[origin, pl.ds(h * span, span)]

    def ring_copy(way, c, s, h):
        origin = lax.rem(z + (nz - s if way == 0 else s), nz)
        to = lax.rem(z + (1 if way == 0 else nz - 1), nz)
        return pltpu.make_async_remote_copy(
            unit(c, origin, h),
            unit(c, origin, h),
            ring_send.at[way],
            ring_recv.at[way, c, s, h],
            device_id={"dp": to},
            device_id_type=MESH,
        )

    def send_own(c, h):
        ring_copy(0, c, 0, h).start()
        ring_copy(1, c, 0, h).start()

    def goes(way, s, h):
        return s < last or (s == last and h * 2 // UNITS == way)

    whole_wait(came_g.at[pl.ds(0, (ns - 1) * cap)], swap_recv.at[0])
    whole_wait(came_p.at[pl.ds(0, (ns - 1) * cap)], swap_recv.at[1])
    for h in range(UNITS):

        @pl.loop(h * span, (h + 1) * span, unroll=UNROLL)
        def _(b):
            slot = slot_of[b]
            factor = col_fac[me, pl.ds(jnp.clip(mats[b], 0, MATS - 1), 1), :]
            pieces[0][z, b, 0] = (came_p[slot].astype(f32) - came_g[slot] * factor).astype(jnp.bfloat16)

        send_own(0, h)

    def swap(c, q):
        return pltpu.make_async_remote_copy(
            updated[c].at[q],
            arrived[c].at[pl.ds(me * cap, cap)],
            swap_send.at[c + 1],
            swap_recv.at[c + 1],
            device_id={"shard": q},
            device_id_type=MESH,
        )

    def update(c):
        low = FIRST[c] * PART // 8 * 8
        high = -(-(FIRST[c] + SIZES[c]) * PART // 8) * 8

        @pl.loop(0, ns)
        def _(k):
            q = lax.rem(me + k, ns)
            at = pl.ds(pl.multiple_of(q * LANES, LANES), LANES)
            for j in range(cap):
                factor = col_fac[q, pl.ds(matrix_of[j], 1), :]
                value = p[j, :, at].astype(f32)[low:high] - g[j, low:high, at] * row_fac[j, low:high] * factor
                for i in range(SIZES[c]):
                    top = (FIRST[c] + i) * PART - low
                    updated[c][q, j, i] = value[top : top + PART].astype(jnp.bfloat16)

            @pl.when(k > 1)
            def _():
                swap(c, lax.rem(me + k - 1, ns)).start()

        swap(c, lax.rem(me + ns - 1, ns)).start()
        for j in range(cap):
            arrived[c][me * cap + j] = updated[c][me, j]

    def compact(c):
        whole_wait(arrived[c].at[pl.ds(0, (ns - 1) * cap)], swap_recv.at[c + 1])
        for h in range(UNITS):

            @pl.loop(h * span, (h + 1) * span, unroll=UNROLL)
            def _(b):
                pieces[c][z, b] = arrived[c][slot_of[b]]

            send_own(c, h)

    def take(c, s):
        for h in range(UNITS):
            for way in range(2):
                if not goes(way, s, h):
                    continue
                origin = lax.rem(z + (nz - 1 - s if way == 0 else 1 + s), nz)
                whole_wait(unit(c, origin, h), ring_recv.at[way, c, s, h])
                if s < last and goes(way, s + 1, h):
                    ring_copy(way, c, s + 1, h).start()

    for c, s in ORDER:
        if s == UPDATE:
            update(c)
        elif s == 0:
            compact(c)
        elif s <= last:
            take(c, s - 1)
    for c in range(CHUNKS):
        take(c, last)

    whole_wait(from_plane.at[pl.ds(0, ns - 1)], small_send.at[0])
    whole_wait(from_line.at[pl.ds(0, nz - 1)], small_send.at[1])
    whole_wait(from_plane.at[pl.ds(0, ns - 1)], small_send.at[2])
    whole_wait(came_g.at[pl.ds(0, (ns - 1) * cap)], swap_send.at[0])
    whole_wait(came_p.at[pl.ds(0, (ns - 1) * cap)], swap_send.at[1])
    for c in range(1, CHUNKS):
        whole_wait(arrived[c].at[pl.ds(0, (ns - 1) * cap)], swap_send.at[c + 1])
    for way in range(2):
        whole_wait(pieces[-1].at[pl.ds(0, sum(SIZES) * (2 * last + 1) // (2 * SIZES[-1]))], ring_send.at[way])


def finish(nz, *refs):
    pieces, (rows, cols, out_params, out_rows, out_cols, sem) = refs[:CHUNKS], refs[CHUNKS:]
    pairs = [(pieces[c].at[s], out_params.at[:, s, pl.ds(FIRST[c], SIZES[c])]) for c in range(CHUNKS) for s in range(nz)]
    pairs += [(rows, out_rows), (cols, out_cols)]
    copies = [pltpu.make_async_copy(source, target, sem.at[i]) for i, (source, target) in enumerate(pairs)]
    for copy in copies:
        copy.start()
    for copy in copies:
        copy.wait()


def body(ns, nz, grad, param, row_state, col_state, block_start, block_matrix, step):
    cap = grad.shape[0]
    nb = block_matrix.shape[0]
    f32, bf16 = jnp.float32, jnp.bfloat16
    dma = pltpu.SemaphoreType.DMA
    vmem = pl.BlockSpec(memory_space=pltpu.VMEM)
    hbm = pl.BlockSpec(memory_space=pltpu.HBM)
    landed = pl.pallas_call(
        functools.partial(kernel, ns, nz, cap, nb),
        out_shape=(
            *[pltpu.VMEM((nz, nb, size, PART, LANES), bf16) for size in SIZES],
            pltpu.VMEM(row_state.shape, f32),
            pltpu.VMEM(col_state.shape, f32),
        ),
        in_specs=[pl.BlockSpec(memory_space=pltpu.SMEM)] + [hbm] * 6,
        out_specs=(vmem,) * (CHUNKS + 2),
        scratch_shapes=[
            pltpu.SMEM(block_start.shape, jnp.int32),
            pltpu.SMEM(block_matrix.shape, jnp.int32),
            pltpu.VMEM(row_state.shape, f32),
            pltpu.VMEM(col_state.shape, f32),
            pltpu.VMEM(grad.shape, f32),
            pltpu.VMEM(param.shape, bf16),
            pltpu.VMEM((ns, 8, LANES), f32),
            pltpu.VMEM((ns, 8, LANES), f32),
            pltpu.VMEM((2, 8, LANES), f32),
            pltpu.VMEM((nz, 8, LANES), f32),
            pltpu.VMEM((ns, 8, LANES), f32),
            pltpu.VMEM((cap, ROWS, LANES), f32),
            pltpu.VMEM((cap, ROWS, LANES), f32),
            pltpu.VMEM((ns, 8, LANES), f32),
            *[pltpu.VMEM((ns, cap, size, PART, LANES), bf16) for size in SIZES[1:]],
            pltpu.VMEM((ns, cap, PART, LANES), f32),
            pltpu.VMEM((ns, cap, PART, LANES), bf16),
            pltpu.VMEM((ns * cap, PART, LANES), f32),
            pltpu.VMEM((ns * cap, PART, LANES), bf16),
            *[pltpu.VMEM((ns * cap, size, PART, LANES), bf16) for size in SIZES[1:]],
            pltpu.SMEM((nb,), jnp.int32),
            pltpu.SMEM((cap * MATS,), f32),
            pltpu.SMEM((cap,), jnp.int32),
            dma((6,)),
            dma((3,)),
            dma((3,)),
            dma((CHUNKS + 1,)),
            dma((CHUNKS + 1,)),
            dma((2,)),
            dma((2, CHUNKS, nz // 2, UNITS)),
        ],
        compiler_params=pltpu.CompilerParams(collective_id=0, has_side_effects=True, vmem_limit_bytes=24 << 20),
        name="step",
    )(step, *(pltpu.with_memory_space_constraint(a, pltpu.HBM) for a in (block_start, block_matrix, grad, param, row_state, col_state)))
    new_params, new_rows, new_cols = pl.pallas_call(
        functools.partial(finish, nz),
        out_shape=(
            jax.ShapeDtypeStruct((nb, nz, ROWS // PART, PART, LANES), bf16),
            jax.ShapeDtypeStruct(row_state.shape, f32),
            jax.ShapeDtypeStruct(col_state.shape, f32),
        ),
        in_specs=[vmem] * (CHUNKS + 2),
        out_specs=(hbm,) * 3,
        scratch_shapes=[dma((CHUNKS * nz + 2,))],
        compiler_params=pltpu.CompilerParams(vmem_limit_bytes=8 << 20),
        name="finish",
    )(*landed)
    return new_params.reshape(nb * nz * ROWS, LANES), new_rows, new_cols


def solution(mesh):
    return jax.shard_map(
        functools.partial(body, mesh.shape["shard"], mesh.shape["dp"]),
        mesh=mesh,
        in_specs=(P("shard", "dp", None), P("shard", "dp", None), P("shard", "dp"), P(), P(), P(), P()),
        out_specs=(P(None, "shard"), P("shard", "dp"), P()),
        check_vma=False,
    )
```

```python
import functools

import jax
import jax.numpy as jnp
from jax import lax
from jax.experimental import pallas as pl
from jax.experimental.pallas import tpu as pltpu
from jax.sharding import PartitionSpec as P

MESH = pl.DeviceIdType.MESH
LANES = 128
ROWS = 16
MATS = 3
PART = 2
SIZES = (1, 1, 2, 4)
FIRST = (0, 1, 2, 4)
CHUNKS = len(SIZES)
UNITS = (4, 2, 2, 4)
UNROLL = 6
UPDATE = -1
ORDER = (
    (1, UPDATE),
    (0, 1),
    (2, UPDATE),
    (0, 2),
    (1, 0),
    (3, UPDATE),
    (0, 3),
    (1, 1),
    (2, 0),
    (1, 2),
    (2, 1),
    (1, 3),
    (2, 2),
    (3, 0),
    (2, 3),
    (3, 1),
    (3, 2),
    (3, 3),
)


def whole_wait(ref, sem):
    pltpu.make_async_copy(ref, ref, sem).wait()


def kernel(
    ns,
    nz,
    cap,
    nb,
    step,
    starts_hbm,
    mats_hbm,
    grad_hbm,
    param_hbm,
    row_state_hbm,
    col_state_hbm,
    pieces_0,
    pieces_1,
    pieces_2,
    pieces_3,
    out_rows,
    out_cols,
    starts,
    mats,
    row_state,
    col_state,
    g,
    p,
    stat,
    from_plane,
    mine,
    from_line,
    totals,
    row_inv,
    row_fac,
    col_fac,
    updated_1,
    updated_2,
    updated_3,
    early_g,
    early_p,
    came_g,
    came_p,
    arrived_1,
    arrived_2,
    arrived_3,
    slot_of,
    weight,
    matrix_of,
    load_sem,
    small_send,
    small_recv,
    swap_send,
    swap_recv,
    ring_send,
    ring_recv,
):
    me = lax.axis_index("shard")
    z = lax.axis_index("dp")
    cols = ns * LANES
    f32 = jnp.float32

    def peer(k):
        return lax.rem(me + k, ns)

    span = [nb // units for units in UNITS]
    last = nz // 2 - 1
    pieces = (pieces_0, pieces_1, pieces_2, pieces_3)
    updated = (None, updated_1, updated_2, updated_3)
    arrived = (None, arrived_1, arrived_2, arrived_3)

    loads = [
        pltpu.make_async_copy(source, target, load_sem.at[i])
        for i, (source, target) in enumerate(
            (
                (starts_hbm, starts),
                (mats_hbm, mats),
                (row_state_hbm, row_state),
                (grad_hbm, g),
                (col_state_hbm, col_state),
                (param_hbm, p),
            )
        )
    ]
    for load in loads[:5]:
        load.start()
    barrier = pltpu.get_barrier_semaphore()

    @pl.loop(1, ns)
    def _(k):
        pl.semaphore_signal(barrier, inc=1, device_id={"shard": peer(k)}, device_id_type=MESH)

    @pl.loop(1, nz)
    def _(k):
        pl.semaphore_signal(barrier, inc=1, device_id={"dp": lax.rem(z + k, nz)}, device_id_type=MESH)

    for load in loads[:3]:
        load.wait()
    first = starts[me]
    owned = jnp.where(me == ns - 1, nb, starts[jnp.minimum(me + 1, ns - 1)]) - first
    for j in range(cap):
        m_of = jnp.clip(mats[jnp.minimum(first + j, nb - 1)], 0, MATS - 1)
        matrix_of[j] = m_of
        for m in range(MATS):
            weight[j * MATS + m] = jnp.where((j < owned) & (m_of == m), 1.0, 0.0).astype(f32)

    t = jnp.full((ROWS, LANES), step[0].astype(f32), f32)
    beta = 1.0 - jnp.exp(-0.8 * jnp.log(t))
    rest = 1.0 - beta
    lr = 1.0 / jnp.sqrt(jnp.maximum(t, 10000.0))
    sub = lax.broadcasted_iota(jnp.int32, (ROWS, ROWS), 0)
    lane = lax.broadcasted_iota(jnp.int32, (ROWS, ROWS), 1)
    eye = sub == lane

    loads[3].wait()
    loads[5].start()
    row_sums = [jnp.zeros((ROWS, 1), f32) for _ in range(MATS)]
    for j in range(cap):
        gj = g[j]
        total = jnp.sum(gj * gj, axis=1, keepdims=True)
        live = jnp.full((ROWS, 1), owned, jnp.int32) > j
        old = jnp.sum(jnp.where(eye, jnp.broadcast_to(row_state[j : j + 1, :], (ROWS, ROWS)), 0.0), axis=1, keepdims=True)
        new = jnp.where(live, beta[:, :1] * old + rest[:, :1] * total / cols, 0.0)
        safe = jnp.where(live, new, 1.0)
        row_inv[j] = jnp.broadcast_to(1.0 / safe, (ROWS, LANES))
        row_fac[j] = jnp.broadcast_to(1.0 / jnp.sqrt(safe), (ROWS, LANES))
        out_rows[j : j + 1, :] = jnp.sum(jnp.where(eye, jnp.broadcast_to(new, (ROWS, ROWS)), 0.0), axis=0, keepdims=True)
        for m in range(MATS):
            row_sums[m] = row_sums[m] + weight[j * MATS + m] * new
    at_lane = lax.broadcasted_iota(jnp.int32, (1, LANES), 1)
    row_line = jnp.zeros((1, LANES), f32)
    for m in range(MATS):
        row_line = jnp.where(at_lane == m, jnp.sum(row_sums[m], axis=0, keepdims=True), row_line)

    @pl.loop(0, ns, unroll=4)
    def _(q):
        at = pl.ds(pl.multiple_of(q * LANES, LANES), LANES)
        acc = [jnp.zeros((8, LANES), f32) for _ in range(2 * MATS)]
        for j in range(cap):
            upper = g[j, 0:8, at]
            lower = g[j, 8:16, at]
            upper, lower = upper * upper, lower * lower
            plain = upper + lower
            quot = upper * row_inv[j, 0:8] + lower * row_inv[j, 8:16]
            for m in range(MATS):
                w = weight[j * MATS + m]
                acc[m] = acc[m] + w * plain
                acc[MATS + m] = acc[MATS + m] + w * quot
        for i in range(2 * MATS):
            stat[q, i : i + 1, :] = jnp.sum(acc[i], axis=0, keepdims=True)
        stat[q, 6:7, :] = row_line
        stat[q, 7:8, :] = jnp.zeros((1, LANES), f32)

    pl.semaphore_wait(barrier, ns - 1 + nz - 1)

    from_plane[me] = stat[me]

    @pl.loop(1, ns)
    def _(k):
        q = peer(k)
        pltpu.make_async_remote_copy(
            stat.at[q], from_plane.at[me], small_send.at[0], small_recv.at[0], device_id={"shard": q}, device_id_type=MESH
        ).start()

    loads[5].wait()

    def early(q):
        return [
            pltpu.make_async_remote_copy(
                source.at[q], target.at[pl.ds(me * cap, cap)], swap_send.at[i], swap_recv.at[i], device_id={"shard": q}, device_id_type=MESH
            )
            for i, (source, target) in enumerate(((early_g, came_g), (early_p, came_p)))
        ]

    def prepare(q, to_g, to_p, first_row):
        at = pl.ds(pl.multiple_of(q * LANES, LANES), LANES)
        for j in range(cap):
            to_g[first_row + j] = (g[j, 0:8, at] * row_fac[j, 0:8])[:PART]
            to_p[first_row + j] = p[j, :, at][:PART]

    prepare(me, came_g, came_p, me * cap)

    @pl.loop(1, ns)
    def _(k):
        q = lax.rem(me + k, ns)
        prepare(q, early_g.at[q], early_p.at[q], 0)

    def place(b, owner):
        following = starts[jnp.minimum(owner + 1, ns - 1)]
        owner = jnp.where((owner < ns - 1) & (following <= b), owner + 1, owner)
        slot_of[b] = owner * cap + jnp.clip(b - starts[owner], 0, cap - 1)
        return owner

    lax.fori_loop(0, nb, place, jnp.int32(0))

    whole_wait(from_plane.at[pl.ds(0, ns - 1)], small_recv.at[0])
    parts = [from_plane[s] for s in range(4)]
    for s in range(4, ns):
        parts[s % 4] = parts[s % 4] + from_plane[s]
    mine[0] = (parts[0] + parts[1]) + (parts[2] + parts[3])
    from_line[z] = mine[0]

    @pl.loop(1, nz)
    def _(k):
        other = lax.rem(z + k, nz)
        pltpu.make_async_remote_copy(
            mine.at[0], from_line.at[z], small_send.at[1], small_recv.at[1], device_id={"dp": other}, device_id_type=MESH
        ).start()

    @pl.loop(1, ns)
    def _(k):
        for copy in early(peer(k)):
            copy.start()

    whole_wait(from_line.at[pl.ds(0, nz - 1)], small_recv.at[1])
    both = from_line[0]
    for s in range(1, nz):
        both = both + from_line[s]
    mine[1] = both
    totals[me] = both

    @pl.loop(1, ns)
    def _(k):
        q = peer(k)
        pltpu.make_async_remote_copy(
            mine.at[1], totals.at[me], small_send.at[2], small_recv.at[2], device_id={"shard": q}, device_id_type=MESH
        ).start()

    loads[4].wait()
    whole_wait(totals.at[pl.ds(0, ns - 1)], small_recv.at[2])

    row_count = jnp.where(lax.broadcasted_iota(jnp.int32, (MATS, LANES), 0) < 2, f32(cols), f32(nb * ROWS * nz - 2 * cols))
    ratio = jnp.zeros((MATS, LANES), f32)
    for q in range(ns):
        at = pl.ds(q * LANES, LANES)
        new = beta[:MATS] * col_state[:, at] + rest[:MATS] * totals[q, 0:MATS, :] / row_count
        out_cols[:, at] = new
        ratio = ratio + totals[q, MATS : 2 * MATS, :] / new
    ratio = jnp.sum(ratio, axis=1, keepdims=True)
    spread = jnp.broadcast_to(totals[0, 6:7, :], (8, LANES))
    on = lax.broadcasted_iota(jnp.int32, (8, LANES), 0) == lax.broadcasted_iota(jnp.int32, (8, LANES), 1)
    row_total = jnp.sum(jnp.where(on, spread, 0.0), axis=1, keepdims=True)[:MATS]
    average = row_total / row_count[:, :1]
    clip = jnp.maximum(1.0, jnp.sqrt(average * ratio / (row_count[:, :1] * cols)))
    scale = lr[:MATS, :1] * jnp.sqrt(average) / clip
    for q in range(ns):
        col_fac[q, 0:MATS, :] = scale / jnp.sqrt(out_cols[:, pl.ds(q * LANES, LANES)])

    def unit(c, origin, h):
        return pieces[c].at[origin, pl.ds(h * span[c], span[c])]

    def goes(way, c, s, h):
        return s < last or (s == last and h * 2 // UNITS[c] == way)

    hops = [(way, c, s, h) for c in range(CHUNKS) for s in range(last + 1) for h in range(UNITS[c]) for way in range(2)]
    arrival = dict(zip((hop for hop in hops if goes(*hop)), range(len(hops)))).__getitem__

    def ring_copy(way, c, s, h):
        origin = lax.rem(z + (nz - s if way == 0 else s), nz)
        to = lax.rem(z + (1 if way == 0 else nz - 1), nz)
        return pltpu.make_async_remote_copy(
            unit(c, origin, h),
            unit(c, origin, h),
            ring_send.at[way],
            ring_recv.at[arrival((way, c, s, h))],
            device_id={"dp": to},
            device_id_type=MESH,
        )

    def send_own(c, h):
        ring_copy(0, c, 0, h).start()
        ring_copy(1, c, 0, h).start()

    whole_wait(came_g.at[pl.ds(0, (ns - 1) * cap)], swap_recv.at[0])
    whole_wait(came_p.at[pl.ds(0, (ns - 1) * cap)], swap_recv.at[1])
    for h in range(UNITS[0]):

        @pl.loop(h * span[0], (h + 1) * span[0], unroll=UNROLL)
        def _(b):
            slot = slot_of[b]
            factor = col_fac[me, pl.ds(jnp.clip(mats[b], 0, MATS - 1), 1), :]
            pieces[0][z, b, 0] = (came_p[slot].astype(f32) - came_g[slot] * factor).astype(jnp.bfloat16)

        send_own(0, h)

    def swap(c, q):
        return pltpu.make_async_remote_copy(
            updated[c].at[q],
            arrived[c].at[pl.ds(me * cap, cap)],
            swap_send.at[c + 1],
            swap_recv.at[c + 1],
            device_id={"shard": q},
            device_id_type=MESH,
        )

    def update(c):
        low = FIRST[c] * PART // 8 * 8
        high = -(-(FIRST[c] + SIZES[c]) * PART // 8) * 8

        @pl.loop(0, ns, unroll=2)
        def _(k):
            q = lax.rem(me + k, ns)
            at = pl.ds(pl.multiple_of(q * LANES, LANES), LANES)
            for j in range(cap):
                factor = col_fac[q, pl.ds(matrix_of[j], 1), :]
                value = p[j, :, at].astype(f32)[low:high] - g[j, low:high, at] * row_fac[j, low:high] * factor
                for i in range(SIZES[c]):
                    top = (FIRST[c] + i) * PART - low
                    updated[c][q, j, i] = value[top : top + PART].astype(jnp.bfloat16)

            @pl.when(k > 1)
            def _():
                swap(c, lax.rem(me + k - 1, ns)).start()

        swap(c, lax.rem(me + ns - 1, ns)).start()
        for j in range(cap):
            arrived[c][me * cap + j] = updated[c][me, j]

    def compact(c):
        whole_wait(arrived[c].at[pl.ds(0, (ns - 1) * cap)], swap_recv.at[c + 1])
        for h in range(UNITS[c]):

            @pl.loop(h * span[c], (h + 1) * span[c], unroll=UNROLL)
            def _(b):
                pieces[c][z, b] = arrived[c][slot_of[b]]

            send_own(c, h)

    def take(c, s):
        for h in range(UNITS[c]):
            for way in range(2):
                if not goes(way, c, s, h):
                    continue
                origin = lax.rem(z + (nz - 1 - s if way == 0 else 1 + s), nz)
                whole_wait(unit(c, origin, h), ring_recv.at[arrival((way, c, s, h))])
                if s < last and goes(way, c, s + 1, h):
                    ring_copy(way, c, s + 1, h).start()

    for c, s in ORDER:
        if s == UPDATE:
            update(c)
        elif s == 0:
            compact(c)
        elif s <= last:
            take(c, s - 1)
    for c in range(CHUNKS):
        take(c, last)

    whole_wait(from_plane.at[pl.ds(0, ns - 1)], small_send.at[0])
    whole_wait(from_line.at[pl.ds(0, nz - 1)], small_send.at[1])
    whole_wait(from_plane.at[pl.ds(0, ns - 1)], small_send.at[2])
    whole_wait(came_g.at[pl.ds(0, (ns - 1) * cap)], swap_send.at[0])
    whole_wait(came_p.at[pl.ds(0, (ns - 1) * cap)], swap_send.at[1])
    for c in range(1, CHUNKS):
        whole_wait(arrived[c].at[pl.ds(0, (ns - 1) * cap)], swap_send.at[c + 1])
    for way in range(2):
        whole_wait(pieces[-1].at[pl.ds(0, sum(SIZES) * (2 * last + 1) // (2 * SIZES[-1]))], ring_send.at[way])


def finish(nz, *refs):
    pieces, (rows, cols, out_params, out_rows, out_cols, sem) = refs[:CHUNKS], refs[CHUNKS:]
    small = [pltpu.make_async_copy(rows, out_rows, sem.at[1]), pltpu.make_async_copy(cols, out_cols, sem.at[2])]
    for copy in small:
        copy.start()
    for c in range(CHUNKS):
        for s in range(nz):
            pltpu.make_async_copy(pieces[c].at[s], out_params.at[:, s, pl.ds(FIRST[c], SIZES[c])], sem.at[0]).start()
    for copy in small:
        copy.wait()
    whole_wait(out_params, sem.at[0])


def body(ns, nz, grad, param, row_state, col_state, block_start, block_matrix, step):
    cap = grad.shape[0]
    nb = block_matrix.shape[0]
    f32, bf16 = jnp.float32, jnp.bfloat16
    dma = pltpu.SemaphoreType.DMA
    vmem = pl.BlockSpec(memory_space=pltpu.VMEM)
    hbm = pl.BlockSpec(memory_space=pltpu.HBM)
    landed = pl.pallas_call(
        functools.partial(kernel, ns, nz, cap, nb),
        out_shape=(
            *[pltpu.VMEM((nz, nb, size, PART, LANES), bf16) for size in SIZES],
            pltpu.VMEM(row_state.shape, f32),
            pltpu.VMEM(col_state.shape, f32),
        ),
        in_specs=[pl.BlockSpec(memory_space=pltpu.SMEM)] + [hbm] * 6,
        out_specs=(vmem,) * (CHUNKS + 2),
        scratch_shapes=[
            pltpu.SMEM(block_start.shape, jnp.int32),
            pltpu.SMEM(block_matrix.shape, jnp.int32),
            pltpu.VMEM(row_state.shape, f32),
            pltpu.VMEM(col_state.shape, f32),
            pltpu.VMEM(grad.shape, f32),
            pltpu.VMEM(param.shape, bf16),
            pltpu.VMEM((ns, 8, LANES), f32),
            pltpu.VMEM((ns, 8, LANES), f32),
            pltpu.VMEM((2, 8, LANES), f32),
            pltpu.VMEM((nz, 8, LANES), f32),
            pltpu.VMEM((ns, 8, LANES), f32),
            pltpu.VMEM((cap, ROWS, LANES), f32),
            pltpu.VMEM((cap, ROWS, LANES), f32),
            pltpu.VMEM((ns, 8, LANES), f32),
            *[pltpu.VMEM((ns, cap, size, PART, LANES), bf16) for size in SIZES[1:]],
            pltpu.VMEM((ns, cap, PART, LANES), f32),
            pltpu.VMEM((ns, cap, PART, LANES), bf16),
            pltpu.VMEM((ns * cap, PART, LANES), f32),
            pltpu.VMEM((ns * cap, PART, LANES), bf16),
            *[pltpu.VMEM((ns * cap, size, PART, LANES), bf16) for size in SIZES[1:]],
            pltpu.SMEM((nb,), jnp.int32),
            pltpu.SMEM((cap * MATS,), f32),
            pltpu.SMEM((cap,), jnp.int32),
            dma((6,)),
            dma((3,)),
            dma((3,)),
            dma((CHUNKS + 1,)),
            dma((CHUNKS + 1,)),
            dma((2,)),
            dma((sum(UNITS) * (nz - 1),)),
        ],
        compiler_params=pltpu.CompilerParams(collective_id=0, has_side_effects=True, vmem_limit_bytes=24 << 20),
        name="step",
    )(step, *(pltpu.with_memory_space_constraint(a, pltpu.HBM) for a in (block_start, block_matrix, grad, param, row_state, col_state)))
    new_params, new_rows, new_cols = pl.pallas_call(
        functools.partial(finish, nz),
        out_shape=(
            jax.ShapeDtypeStruct((nb, nz, ROWS // PART, PART, LANES), bf16),
            jax.ShapeDtypeStruct(row_state.shape, f32),
            jax.ShapeDtypeStruct(col_state.shape, f32),
        ),
        in_specs=[vmem] * (CHUNKS + 2),
        out_specs=(hbm,) * 3,
        scratch_shapes=[dma((3,))],
        compiler_params=pltpu.CompilerParams(vmem_limit_bytes=8 << 20),
        name="finish",
    )(*landed)
    return new_params.reshape(nb * nz * ROWS, LANES), new_rows, new_cols


def solution(mesh):
    return jax.shard_map(
        functools.partial(body, mesh.shape["shard"], mesh.shape["dp"]),
        mesh=mesh,
        in_specs=(P("shard", "dp", None), P("shard", "dp", None), P("shard", "dp"), P(), P(), P(), P()),
        out_specs=(P(None, "shard"), P("shard", "dp"), P()),
        check_vma=False,
    )
```

```python
import functools

import jax
import jax.numpy as jnp
from jax import lax
from jax.experimental import pallas as pl
from jax.experimental.pallas import tpu as pltpu
from jax.sharding import PartitionSpec as P

MESH = pl.DeviceIdType.MESH
LANES = 128
ROWS = 16
MATS = 3
PART = 2
SIZES = (1, 1, 2, 4)
FIRST = (0, 1, 2, 4)
CHUNKS = len(SIZES)
UNITS = (4, 2, 2, 4)
UNROLL = 12
UPDATE = -1
ORDER = (
    (1, UPDATE),
    (0, 1),
    (2, UPDATE),
    (0, 2),
    (1, 0),
    (3, UPDATE),
    (0, 3),
    (1, 1),
    (2, 0),
    (1, 2),
    (2, 1),
    (1, 3),
    (2, 2),
    (3, 0),
    (2, 3),
    (3, 1),
    (3, 2),
    (3, 3),
)


def whole_wait(ref, sem):
    pltpu.make_async_copy(ref, ref, sem).wait()


def kernel(
    ns,
    nz,
    cap,
    nb,
    step,
    starts_hbm,
    mats_hbm,
    grad_hbm,
    param_hbm,
    row_state_hbm,
    col_state_hbm,
    pieces_0,
    pieces_1,
    pieces_2,
    pieces_3,
    out_rows,
    out_cols,
    starts,
    mats,
    row_state,
    col_state,
    g,
    p,
    stat,
    from_plane,
    mine,
    from_line,
    totals,
    row_inv,
    row_fac,
    col_fac,
    updated_1,
    updated_2,
    updated_3,
    early_g,
    early_p,
    came_g,
    came_p,
    arrived_1,
    arrived_2,
    arrived_3,
    slot_of,
    weight,
    matrix_of,
    load_sem,
    small_send,
    small_recv,
    swap_send,
    swap_recv,
    ring_send,
    ring_recv,
):
    me = lax.axis_index("shard")
    z = lax.axis_index("dp")
    cols = ns * LANES
    f32 = jnp.float32

    def peer(k):
        return lax.rem(me + k, ns)

    span = [nb // units for units in UNITS]
    last = nz // 2 - 1
    pieces = (pieces_0, pieces_1, pieces_2, pieces_3)
    updated = (None, updated_1, updated_2, updated_3)
    arrived = (None, arrived_1, arrived_2, arrived_3)

    loads = [
        pltpu.make_async_copy(source, target, load_sem.at[i])
        for i, (source, target) in enumerate(
            (
                (starts_hbm, starts),
                (mats_hbm, mats),
                (row_state_hbm, row_state),
                (grad_hbm, g),
                (col_state_hbm, col_state),
                (param_hbm, p),
            )
        )
    ]
    for load in loads[:5]:
        load.start()
    barrier = pltpu.get_barrier_semaphore()

    @pl.loop(1, ns)
    def _(k):
        pl.semaphore_signal(barrier, inc=1, device_id={"shard": peer(k)}, device_id_type=MESH)

    @pl.loop(1, nz)
    def _(k):
        pl.semaphore_signal(barrier, inc=1, device_id={"dp": lax.rem(z + k, nz)}, device_id_type=MESH)

    for load in loads[:3]:
        load.wait()
    first = starts[me]
    owned = jnp.where(me == ns - 1, nb, starts[jnp.minimum(me + 1, ns - 1)]) - first
    for j in range(cap):
        m_of = jnp.clip(mats[jnp.minimum(first + j, nb - 1)], 0, MATS - 1)
        matrix_of[j] = m_of
        for m in range(MATS):
            weight[j * MATS + m] = jnp.where((j < owned) & (m_of == m), 1.0, 0.0).astype(f32)

    t = jnp.full((ROWS, LANES), step[0].astype(f32), f32)
    beta = 1.0 - jnp.exp(-0.8 * jnp.log(t))
    rest = 1.0 - beta
    lr = 1.0 / jnp.sqrt(jnp.maximum(t, 10000.0))
    sub = lax.broadcasted_iota(jnp.int32, (ROWS, ROWS), 0)
    lane = lax.broadcasted_iota(jnp.int32, (ROWS, ROWS), 1)
    eye = sub == lane

    loads[3].wait()
    loads[5].start()
    row_sums = [jnp.zeros((ROWS, 1), f32) for _ in range(MATS)]
    for j in range(cap):
        gj = g[j]
        total = jnp.sum(gj * gj, axis=1, keepdims=True)
        live = jnp.full((ROWS, 1), owned, jnp.int32) > j
        old = jnp.sum(jnp.where(eye, jnp.broadcast_to(row_state[j : j + 1, :], (ROWS, ROWS)), 0.0), axis=1, keepdims=True)
        new = jnp.where(live, beta[:, :1] * old + rest[:, :1] * total / cols, 0.0)
        safe = jnp.where(live, new, 1.0)
        row_inv[j] = jnp.broadcast_to(1.0 / safe, (ROWS, LANES))
        row_fac[j] = jnp.broadcast_to(1.0 / jnp.sqrt(safe), (ROWS, LANES))
        out_rows[j : j + 1, :] = jnp.sum(jnp.where(eye, jnp.broadcast_to(new, (ROWS, ROWS)), 0.0), axis=0, keepdims=True)
        for m in range(MATS):
            row_sums[m] = row_sums[m] + weight[j * MATS + m] * new
    at_lane = lax.broadcasted_iota(jnp.int32, (1, LANES), 1)
    row_line = jnp.zeros((1, LANES), f32)
    for m in range(MATS):
        row_line = jnp.where(at_lane == m, jnp.sum(row_sums[m], axis=0, keepdims=True), row_line)

    @pl.loop(0, ns, unroll=8)
    def _(q):
        at = pl.ds(pl.multiple_of(q * LANES, LANES), LANES)
        acc = [jnp.zeros((8, LANES), f32) for _ in range(2 * MATS)]
        for j in range(cap):
            upper = g[j, 0:8, at]
            lower = g[j, 8:16, at]
            upper, lower = upper * upper, lower * lower
            plain = upper + lower
            quot = upper * row_inv[j, 0:8] + lower * row_inv[j, 8:16]
            for m in range(MATS):
                w = weight[j * MATS + m]
                acc[m] = acc[m] + w * plain
                acc[MATS + m] = acc[MATS + m] + w * quot
        for i in range(2 * MATS):
            stat[q, i : i + 1, :] = jnp.sum(acc[i], axis=0, keepdims=True)
        stat[q, 6:7, :] = row_line
        stat[q, 7:8, :] = jnp.zeros((1, LANES), f32)

    pl.semaphore_wait(barrier, ns - 1 + nz - 1)

    from_plane[me] = stat[me]

    @pl.loop(1, ns)
    def _(k):
        q = peer(k)
        pltpu.make_async_remote_copy(
            stat.at[q], from_plane.at[me], small_send.at[0], small_recv.at[0], device_id={"shard": q}, device_id_type=MESH
        ).start()

    loads[5].wait()

    def early(q):
        return [
            pltpu.make_async_remote_copy(
                source.at[q], target.at[pl.ds(me * cap, cap)], swap_send.at[i], swap_recv.at[i], device_id={"shard": q}, device_id_type=MESH
            )
            for i, (source, target) in enumerate(((early_g, came_g), (early_p, came_p)))
        ]

    def prepare(q, to_g, to_p, first_row):
        at = pl.ds(pl.multiple_of(q * LANES, LANES), LANES)
        for j in range(cap):
            to_g[first_row + j] = (g[j, 0:8, at] * row_fac[j, 0:8])[:PART]
            to_p[first_row + j] = p[j, :, at][:PART]

    prepare(me, came_g, came_p, me * cap)

    @pl.loop(1, ns)
    def _(k):
        q = lax.rem(me + k, ns)
        prepare(q, early_g.at[q], early_p.at[q], 0)

    def place(b, owner):
        following = starts[jnp.minimum(owner + 1, ns - 1)]
        owner = jnp.where((owner < ns - 1) & (following <= b), owner + 1, owner)
        slot_of[b] = owner * cap + jnp.clip(b - starts[owner], 0, cap - 1)
        return owner

    lax.fori_loop(0, nb, place, jnp.int32(0))

    whole_wait(from_plane.at[pl.ds(0, ns - 1)], small_recv.at[0])
    parts = [from_plane[s] for s in range(4)]
    for s in range(4, ns):
        parts[s % 4] = parts[s % 4] + from_plane[s]
    mine[0] = (parts[0] + parts[1]) + (parts[2] + parts[3])
    from_line[z] = mine[0]

    @pl.loop(1, nz)
    def _(k):
        other = lax.rem(z + k, nz)
        pltpu.make_async_remote_copy(
            mine.at[0], from_line.at[z], small_send.at[1], small_recv.at[1], device_id={"dp": other}, device_id_type=MESH
        ).start()

    @pl.loop(1, ns)
    def _(k):
        for copy in early(peer(k)):
            copy.start()

    whole_wait(from_line.at[pl.ds(0, nz - 1)], small_recv.at[1])
    both = from_line[0]
    for s in range(1, nz):
        both = both + from_line[s]
    mine[1] = both
    totals[me] = both

    @pl.loop(1, ns)
    def _(k):
        q = peer(k)
        pltpu.make_async_remote_copy(
            mine.at[1], totals.at[me], small_send.at[2], small_recv.at[2], device_id={"shard": q}, device_id_type=MESH
        ).start()

    loads[4].wait()
    whole_wait(totals.at[pl.ds(0, ns - 1)], small_recv.at[2])

    row_count = jnp.where(lax.broadcasted_iota(jnp.int32, (MATS, LANES), 0) < 2, f32(cols), f32(nb * ROWS * nz - 2 * cols))
    ratio = jnp.zeros((MATS, LANES), f32)
    for q in range(ns):
        at = pl.ds(q * LANES, LANES)
        new = beta[:MATS] * col_state[:, at] + rest[:MATS] * totals[q, 0:MATS, :] / row_count
        out_cols[:, at] = new
        ratio = ratio + totals[q, MATS : 2 * MATS, :] / new
    ratio = jnp.sum(ratio, axis=1, keepdims=True)
    spread = jnp.broadcast_to(totals[0, 6:7, :], (8, LANES))
    on = lax.broadcasted_iota(jnp.int32, (8, LANES), 0) == lax.broadcasted_iota(jnp.int32, (8, LANES), 1)
    row_total = jnp.sum(jnp.where(on, spread, 0.0), axis=1, keepdims=True)[:MATS]
    average = row_total / row_count[:, :1]
    clip = jnp.maximum(1.0, jnp.sqrt(average * ratio / (row_count[:, :1] * cols)))
    scale = lr[:MATS, :1] * jnp.sqrt(average) / clip
    for q in range(ns):
        col_fac[q, 0:MATS, :] = scale / jnp.sqrt(out_cols[:, pl.ds(q * LANES, LANES)])

    def unit(c, origin, h):
        return pieces[c].at[origin, pl.ds(h * span[c], span[c])]

    def goes(way, c, s, h):
        return s < last or (s == last and h * 2 // UNITS[c] == way)

    hops = [(way, c, s, h) for c in range(CHUNKS) for s in range(last + 1) for h in range(UNITS[c]) for way in range(2)]
    arrival = dict(zip((hop for hop in hops if goes(*hop)), range(len(hops)))).__getitem__

    def ring_copy(way, c, s, h):
        origin = lax.rem(z + (nz - s if way == 0 else s), nz)
        to = lax.rem(z + (1 if way == 0 else nz - 1), nz)
        return pltpu.make_async_remote_copy(
            unit(c, origin, h),
            unit(c, origin, h),
            ring_send.at[way],
            ring_recv.at[arrival((way, c, s, h))],
            device_id={"dp": to},
            device_id_type=MESH,
        )

    def send_own(c, h):
        ring_copy(0, c, 0, h).start()
        ring_copy(1, c, 0, h).start()

    whole_wait(came_g.at[pl.ds(0, (ns - 1) * cap)], swap_recv.at[0])
    whole_wait(came_p.at[pl.ds(0, (ns - 1) * cap)], swap_recv.at[1])
    for h in range(UNITS[0]):

        @pl.loop(h * span[0], (h + 1) * span[0], unroll=UNROLL)
        def _(b):
            slot = slot_of[b]
            factor = col_fac[me, pl.ds(jnp.clip(mats[b], 0, MATS - 1), 1), :]
            pieces[0][z, b, 0] = (came_p[slot].astype(f32) - came_g[slot] * factor).astype(jnp.bfloat16)

        send_own(0, h)

    def swap(c, q):
        return pltpu.make_async_remote_copy(
            updated[c].at[q],
            arrived[c].at[pl.ds(me * cap, cap)],
            swap_send.at[c + 1],
            swap_recv.at[c + 1],
            device_id={"shard": q},
            device_id_type=MESH,
        )

    def update(c):
        low = FIRST[c] * PART // 8 * 8
        high = -(-(FIRST[c] + SIZES[c]) * PART // 8) * 8

        @pl.loop(0, ns, unroll=2)
        def _(k):
            q = lax.rem(me + k, ns)
            at = pl.ds(pl.multiple_of(q * LANES, LANES), LANES)
            for j in range(cap):
                factor = col_fac[q, pl.ds(matrix_of[j], 1), :]
                value = p[j, :, at].astype(f32)[low:high] - g[j, low:high, at] * row_fac[j, low:high] * factor
                for i in range(SIZES[c]):
                    top = (FIRST[c] + i) * PART - low
                    updated[c][q, j, i] = value[top : top + PART].astype(jnp.bfloat16)

            @pl.when(k > 1)
            def _():
                swap(c, lax.rem(me + k - 1, ns)).start()

        swap(c, lax.rem(me + ns - 1, ns)).start()
        for j in range(cap):
            arrived[c][me * cap + j] = updated[c][me, j]

    def compact(c):
        whole_wait(arrived[c].at[pl.ds(0, (ns - 1) * cap)], swap_recv.at[c + 1])
        for h in range(UNITS[c]):

            @pl.loop(h * span[c], (h + 1) * span[c], unroll=UNROLL)
            def _(b):
                pieces[c][z, b] = arrived[c][slot_of[b]]

            send_own(c, h)

    def take(c, s):
        for h in range(UNITS[c]):
            for way in range(2):
                if not goes(way, c, s, h):
                    continue
                origin = lax.rem(z + (nz - 1 - s if way == 0 else 1 + s), nz)
                whole_wait(unit(c, origin, h), ring_recv.at[arrival((way, c, s, h))])
                if s < last and goes(way, c, s + 1, h):
                    ring_copy(way, c, s + 1, h).start()

    for c, s in ORDER:
        if s == UPDATE:
            update(c)
        elif s == 0:
            compact(c)
        elif s <= last:
            take(c, s - 1)
    for c in range(CHUNKS):
        take(c, last)

    whole_wait(from_plane.at[pl.ds(0, ns - 1)], small_send.at[0])
    whole_wait(from_line.at[pl.ds(0, nz - 1)], small_send.at[1])
    whole_wait(from_plane.at[pl.ds(0, ns - 1)], small_send.at[2])
    whole_wait(came_g.at[pl.ds(0, (ns - 1) * cap)], swap_send.at[0])
    whole_wait(came_p.at[pl.ds(0, (ns - 1) * cap)], swap_send.at[1])
    for c in range(1, CHUNKS):
        whole_wait(arrived[c].at[pl.ds(0, (ns - 1) * cap)], swap_send.at[c + 1])
    for way in range(2):
        whole_wait(pieces[-1].at[pl.ds(0, sum(SIZES) * (2 * last + 1) // (2 * SIZES[-1]))], ring_send.at[way])


def finish(nz, *refs):
    pieces, (rows, cols, out_params, out_rows, out_cols, sem) = refs[:CHUNKS], refs[CHUNKS:]
    small = [pltpu.make_async_copy(rows, out_rows, sem.at[1]), pltpu.make_async_copy(cols, out_cols, sem.at[2])]
    for copy in small:
        copy.start()
    for c in range(CHUNKS):
        for s in range(nz):
            pltpu.make_async_copy(pieces[c].at[s], out_params.at[:, s, pl.ds(FIRST[c], SIZES[c])], sem.at[0]).start()
    for copy in small:
        copy.wait()
    whole_wait(out_params, sem.at[0])


def body(ns, nz, grad, param, row_state, col_state, block_start, block_matrix, step):
    cap = grad.shape[0]
    nb = block_matrix.shape[0]
    f32, bf16 = jnp.float32, jnp.bfloat16
    dma = pltpu.SemaphoreType.DMA
    vmem = pl.BlockSpec(memory_space=pltpu.VMEM)
    hbm = pl.BlockSpec(memory_space=pltpu.HBM)
    landed = pl.pallas_call(
        functools.partial(kernel, ns, nz, cap, nb),
        out_shape=(
            *[pltpu.VMEM((nz, nb, size, PART, LANES), bf16) for size in SIZES],
            pltpu.VMEM(row_state.shape, f32),
            pltpu.VMEM(col_state.shape, f32),
        ),
        in_specs=[pl.BlockSpec(memory_space=pltpu.SMEM)] + [hbm] * 6,
        out_specs=(vmem,) * (CHUNKS + 2),
        scratch_shapes=[
            pltpu.SMEM(block_start.shape, jnp.int32),
            pltpu.SMEM(block_matrix.shape, jnp.int32),
            pltpu.VMEM(row_state.shape, f32),
            pltpu.VMEM(col_state.shape, f32),
            pltpu.VMEM(grad.shape, f32),
            pltpu.VMEM(param.shape, bf16),
            pltpu.VMEM((ns, 8, LANES), f32),
            pltpu.VMEM((ns, 8, LANES), f32),
            pltpu.VMEM((2, 8, LANES), f32),
            pltpu.VMEM((nz, 8, LANES), f32),
            pltpu.VMEM((ns, 8, LANES), f32),
            pltpu.VMEM((cap, ROWS, LANES), f32),
            pltpu.VMEM((cap, ROWS, LANES), f32),
            pltpu.VMEM((ns, 8, LANES), f32),
            *[pltpu.VMEM((ns, cap, size, PART, LANES), bf16) for size in SIZES[1:]],
            pltpu.VMEM((ns, cap, PART, LANES), f32),
            pltpu.VMEM((ns, cap, PART, LANES), bf16),
            pltpu.VMEM((ns * cap, PART, LANES), f32),
            pltpu.VMEM((ns * cap, PART, LANES), bf16),
            *[pltpu.VMEM((ns * cap, size, PART, LANES), bf16) for size in SIZES[1:]],
            pltpu.SMEM((nb,), jnp.int32),
            pltpu.SMEM((cap * MATS,), f32),
            pltpu.SMEM((cap,), jnp.int32),
            dma((6,)),
            dma((3,)),
            dma((3,)),
            dma((CHUNKS + 1,)),
            dma((CHUNKS + 1,)),
            dma((2,)),
            dma((sum(UNITS) * (nz - 1),)),
        ],
        compiler_params=pltpu.CompilerParams(collective_id=0, has_side_effects=True, vmem_limit_bytes=24 << 20),
        name="step",
    )(step, *(pltpu.with_memory_space_constraint(a, pltpu.HBM) for a in (block_start, block_matrix, grad, param, row_state, col_state)))
    new_params, new_rows, new_cols = pl.pallas_call(
        functools.partial(finish, nz),
        out_shape=(
            jax.ShapeDtypeStruct((nb, nz, ROWS // PART, PART, LANES), bf16),
            jax.ShapeDtypeStruct(row_state.shape, f32),
            jax.ShapeDtypeStruct(col_state.shape, f32),
        ),
        in_specs=[vmem] * (CHUNKS + 2),
        out_specs=(hbm,) * 3,
        scratch_shapes=[dma((3,))],
        compiler_params=pltpu.CompilerParams(vmem_limit_bytes=8 << 20),
        name="finish",
    )(*landed)
    return new_params.reshape(nb * nz * ROWS, LANES), new_rows, new_cols


def solution(mesh):
    return jax.shard_map(
        functools.partial(body, mesh.shape["shard"], mesh.shape["dp"]),
        mesh=mesh,
        in_specs=(P("shard", "dp", None), P("shard", "dp", None), P("shard", "dp"), P(), P(), P(), P()),
        out_specs=(P(None, "shard"), P("shard", "dp"), P()),
        check_vma=False,
    )
```
